128 devices in a mesh: vocab: 64 (over y, x, z), batch: 2 (over core).
Axes of the slice: x: 4, y: 4, z: 4, core: 2. Of those that a mesh axis runs over, the one named last changes fastest.
Arguments:
- hidden: bfloat16 [2048, 7168], P(('batch', 'vocab')), parts along dimension 0, may hold values from -1000 to 1000
- norm_gain: bfloat16 [7168], replicated, may hold values from 1.5 to 5
- lm_head: bfloat16 [7168, 65536], P(None, 'vocab'), may hold values from -2 to 2
- draft_logits: bfloat16 [2048, 65536], P('batch', 'vocab'), parts along dimension 0, may hold values from -480 to 480
- draft_tokens: int32 [2048], P('batch'), parts along dimension 0, may hold values from 0 to 65535
- tree_parents: int32 [2048], P('batch'), parts along dimension 0, may hold values from 0 to 62, as said below
- node_depths: int32 [2048], P('batch'), parts along dimension 0, may hold values from 0 to 8, as said below
- uniforms: float32 [2048], P('batch'), parts along dimension 0, may hold values from 0 to 1
Outputs:
- target_lse: float32 [2048], P('batch'), parts along dimension 0
- token_logprob: float32 [2048], P('batch'), parts along dimension 0
- residual_mass: float32 [2048], P('batch'), parts along dimension 0
- accept_margin: float32 [2048], P('batch'), parts along dimension 0
- path_margin: float32 [2048], P('batch'), parts along dimension 0
The draws below stay inside these ranges and needn't reach their ends.
There are 2 independent parts, one for each index of `batch`. The reference program is written for one: setup_inputs(seed, part) draws one part's arguments, and reference() takes and returns one part's arrays. A program takes and returns all parts, laid end to end along the dimension named above; an argument that names none is the same for every part. Nothing has to cross between parts.
Inputs may be any that keep to these rules, and one draw needn't show every extreme that they name: `tree_parents`: rows come in 16 requests of 64 consecutive rows, the first of each being the root. A node's entry is the position of its parent within the request, smaller than its own position; the root's entry is 0. `node_depths`: A node's depth is its parent's depth plus one, the root's is 0; in every request some node has depth 8.
All inputs are finite; a program needn't handle non-finite values.
Results may differ from the reference program's by a relative error of at most 0.0049.
Values may be sent and summed in bfloat16 or wider, within the bound.
A program may use at most 128 MiB of HBM per device.

```python
import math
import jax
import jax.numpy as jnp
import numpy as np
from jax import lax

D = 7168
VOCAB = 65536
NODES = 64
DEPTH_MAX = 8
REQ = 16
ROWS = 1024


def draw_hidden(key, part):
    gaussian = jax.random.normal(jax.random.fold_in(key, 11), (ROWS, D), jnp.float32)
    return jnp.clip(gaussian, -6.0, 6.0).astype(jnp.bfloat16)


def draw_lm_head(key, part):
    gaussian = jax.random.normal(jax.random.fold_in(key, 21), (D, VOCAB), jnp.float32)
    columns = jnp.arange(VOCAB, dtype=jnp.int32)
    position = columns.astype(jnp.float32) / VOCAB
    weights = gaussian * (1.0 + 0.1 * position) / math.sqrt(D)
    return jnp.clip(weights, -2.0, 2.0).astype(jnp.bfloat16)


def draw_draft_logits(key, part):
    gaussian = jax.random.normal(jax.random.fold_in(key, 31), (ROWS, VOCAB), jnp.float32)
    columns = jnp.arange(VOCAB, dtype=jnp.int32)
    position = columns.astype(jnp.float32) / VOCAB
    return jnp.clip(3.0 * gaussian * (1.0 + 0.1 * position), -24.0, 24.0).astype(jnp.bfloat16)


def build_tree(key):
    jitter = jax.random.randint(jax.random.fold_in(key, 41), (REQ, NODES, NODES), 0, 4096)
    positions = jnp.arange(NODES, dtype=jnp.int32)

    def grow_tree(jitter_request):

        def add_node(carry, node_index):
            depths, deepest = carry
            eligible = (positions < node_index) & (depths < DEPTH_MAX)
            forced = NODES - node_index <= DEPTH_MAX - deepest
            ranked = jnp.where(forced, depths * 65536 + positions, (jitter_request[node_index] + 1024 * depths) * 64 + positions)
            ranked = jnp.where(eligible, ranked, -1)
            chosen_parent = jnp.argmax(ranked).astype(jnp.int32)
            new_depth = depths[chosen_parent] + 1
            depths = depths.at[node_index].set(new_depth)
            return ((depths, jnp.maximum(deepest, new_depth)), (chosen_parent, new_depth))
        initial = (jnp.zeros((NODES,), jnp.int32), jnp.int32(0))
        _, (parents, depths) = lax.scan(add_node, initial, jnp.arange(1, NODES, dtype=jnp.int32))
        anchor = jnp.zeros((1,), jnp.int32)
        return (jnp.concatenate([anchor, parents]), jnp.concatenate([anchor, depths]))
    parents, depths = jax.vmap(grow_tree)(jitter)
    return (parents.reshape(ROWS).astype(jnp.int32), depths.reshape(ROWS).astype(jnp.int32))


def draw_tree_parents(key, part):
    return build_tree(key)[0]


def draw_node_depths(key, part):
    return build_tree(key)[1]


def set_ends(values, rng, low, largest):
    longest = values.shape.index(max(values.shape))
    spots = []
    for shift in (0, 1):
        where = [jax.random.randint(jax.random.fold_in(rng, axis), (), 0, length) for axis, length in enumerate(values.shape)]
        where[longest] = (where[longest] + shift) % values.shape[longest]
        spots.append(tuple(where))
    return values.at[spots[0]].set(low).at[spots[1]].set(largest)


def cumulative_ranks(amount, lean):
    loads = [(1 << 20) // math.isqrt(rank ** lean) + 1 for rank in range(1, amount + 1)]
    width = 1 + sum(loads) // (1 << 30)
    return np.cumsum(np.array([max(1, weight // width) for weight in loads]))


def ranked_ids(rng, dims, number_of, slope):
    grid = cumulative_ranks(number_of, slope)
    lot = jax.random.randint(jax.random.fold_in(rng, 1), dims, 0, int(grid[number_of - 1]))
    standing = jnp.searchsorted(jnp.asarray(grid, jnp.int32), lot, side="right")
    return jax.random.permutation(jax.random.fold_in(rng, 2), number_of)[standing].astype(jnp.int32)


def setup_inputs(seed: int = 0, part: int = 0) -> dict:
    key_list = jax.random.split(jax.random.key(seed), 9)
    part_splits = jax.random.split(jax.random.fold_in(key_list[8], part), 9)
    return {
        "hidden": draw_hidden(jax.random.fold_in(jax.random.fold_in(key_list[8], part), 71), part),
        "norm_gain": jnp.clip(jnp.exp(jax.random.uniform(key_list[1], (D,), jnp.float32, math.log(1.5), math.log(5.0))), 1.5, 5.0).astype(jnp.bfloat16),
        "lm_head": draw_lm_head(jax.random.fold_in(key_list[8], 71), part),
        "draft_logits": draw_draft_logits(jax.random.fold_in(jax.random.fold_in(key_list[8], part), 71), part),
        "draft_tokens": set_ends(ranked_ids(part_splits[4], (ROWS,), VOCAB, 2), jax.random.fold_in(part_splits[4], 3), 0, VOCAB - 1).astype(jnp.int32),
        "tree_parents": draw_tree_parents(jax.random.fold_in(jax.random.fold_in(key_list[8], part), 71), part),
        "node_depths": draw_node_depths(jax.random.fold_in(jax.random.fold_in(key_list[8], part), 71), part),
        "uniforms": jnp.clip(jax.random.uniform(part_splits[7], (ROWS,), jnp.float32, 0.0, 1.0), 0.0, 1.0),
    }


epsilon = 1e-06

def normalize(hidden_rows, gain_vector):
    values = hidden_rows.astype(jnp.float32)
    mean_square = lax.optimization_barrier(jnp.mean(values * values, axis=1, keepdims=True))
    scaled = values * lax.rsqrt(mean_square + epsilon) * gain_vector.astype(jnp.float32)
    return scaled.astype(jnp.bfloat16)

def log_total(scores):
    row_max = lax.optimization_barrier(jnp.max(scores, axis=1))
    return row_max + jnp.log(lax.optimization_barrier(jnp.sum(jnp.exp(scores - row_max[:, None]), axis=1)))

def reference(hidden, norm_gain, lm_head, draft_logits, draft_tokens, tree_parents, node_depths, uniforms):
    normed = normalize(hidden, norm_gain)
    logits = jnp.dot(normed, lm_head, preferred_element_type=jnp.float32)
    draft_values = draft_logits.astype(jnp.float32)
    target_lse = log_total(logits)
    draft_lse = log_total(draft_values)
    positions = jnp.arange(ROWS, dtype=jnp.int32)
    parent_row = (positions - positions % NODES + tree_parents).astype(jnp.int32)
    token_logprob = logits[parent_row, draft_tokens] - target_lse[parent_row]
    draft_logprob = draft_values[parent_row, draft_tokens] - draft_lse[parent_row]
    accept_margin = jnp.exp(jnp.minimum(token_logprob - draft_logprob, 0.0)) - uniforms
    target_prob = jnp.exp(logits - target_lse[:, None])
    draft_prob = jnp.exp(draft_values - draft_lse[:, None])
    residual_mass = lax.optimization_barrier(jnp.sum(jnp.maximum(target_prob - draft_prob, 0.0), axis=1))
    path_margin = jnp.ones((ROWS,), jnp.float32)
    for level_now in range(1, DEPTH_MAX + 1):
        path_margin = jnp.where(node_depths == level_now, jnp.minimum(accept_margin, path_margin[parent_row]), path_margin)
    return (target_lse, token_logprob, residual_mass, accept_margin, path_margin)
```

```python
import heapq
import itertools

import jax
import jax.numpy as jnp
from jax import lax
from jax.experimental import pallas as pl
from jax.experimental.pallas import tpu as pltpu
from jax.sharding import PartitionSpec as P

NODES = 64
DEPTH_MAX = 8
EPSILON = 1e-06
LANES = 128
SIDE = 4
MESH = pl.DeviceIdType.MESH

ROUTES = ((0, 1, 2), (1, 2, 0), (2, 0, 1))
GROUPS = ((2, 4, 4, 4, 4, 1), (2, 4, 4, 4, 4, 1), (2, 4, 4, 4, 3, 1))


def relay_sides():
    sides = {}
    for p, sizes in enumerate(GROUPS):
        for phase in range(3):
            lean = 0
            for g in sorted(range(len(sizes)), key=lambda g: -sizes[g]):
                sides[p, g, phase] = 0 if lean <= 0 else 1
                lean += sizes[g] if lean <= 0 else -sizes[g]
    return sides


SIDES = relay_sides()


def plan():
    rate, latency = 46600.0, 2.2
    free = {(a, d): 0.0 for a in range(3) for d in range(2)}
    coming, count, have, order, ready = [], itertools.count(), set(), [], []

    def send(now, p, g, phase, kind):
        way = (ROUTES[p][phase], kind if kind < 2 else SIDES[p, g, phase])
        free[way] = max(now, free[way]) + GROUPS[p][g] * 4096 * SIDE**phase / rate
        heapq.heappush(coming, (free[way] + latency, next(count), (p, g, phase, kind)))

    now = 0.0
    for g in range(max(map(len, GROUPS))):
        for p in range(3):
            if g < len(GROUPS[p]):
                send(now, p, g, 0, 0)
                send(now, p, g, 0, 1)
    while coming or ready:
        if coming and (coming[0][0] <= now or not ready):
            at, _, message = heapq.heappop(coming)
            now = max(now, at) + 0.03
            p, g, phase, kind = message
            have.add(message)
            order.append(("take", message))
            if kind == SIDES[p, g, phase]:
                send(now, p, g, phase, 2)
            if all((p, g, phase, k) in have for k in range(3)):
                if phase < 2:
                    send(now, p, g, phase + 1, 0)
                    send(now, p, g, phase + 1, 1)
                else:
                    ready.append((p, g))
        else:
            p, g = ready.pop(0)
            order.append(("multiply", (p, g)))
            now += 0.27 * max(2, GROUPS[p][g])
    return order


ORDER = plan()
PAIRS = [(p, g) for kind, (p, g, *_) in ORDER if kind == "multiply"]
MESSAGES = [m for kind, m in ORDER if kind == "take"]
FIRST_TILE = {
    (p, g): sum(map(sum, GROUPS[:p])) + sum(GROUPS[p][:g]) for p in range(3) for g in range(len(GROUPS[p]))
}


def as_column(row):
    return jnp.transpose(jnp.broadcast_to(row, (LANES, LANES)))


def main_kernel(
    hidden_hbm, gain_hbm, head_hbm, draft_hbm, tokens_hbm, parents_hbm,
    out_ref,
    hidden_ref, gain_ref, head_ref, draft_ref, tokens_ref, parents_ref,
    rows_ref, logits_ref, weight_ref, draft_prob_ref, stat_ref, pair_ref, triple_ref,
    small_sem, head_sem, send_sem, take_sem, swap_send_sem, swap_take_sem,
):
    me = lax.axis_index("vocab")
    batch = lax.axis_index("batch")
    at = (me // 16, (me // 4) % 4, me % 4)
    stride = (16, 4, 1)
    width = logits_ref.shape[1]
    spans = logits_ref.shape[0] // LANES

    def peer(axis, step):
        return (me + (lax.rem(at[axis] + step, SIDE) - at[axis]) * stride[axis], batch)

    small = [
        pltpu.make_async_copy(src, dst, small_sem.at[k])
        for k, (src, dst) in enumerate(
            (
                (hidden_hbm, hidden_ref),
                (gain_hbm, gain_ref),
                (draft_hbm, draft_ref),
                (tokens_hbm, tokens_ref),
                (parents_hbm, parents_ref),
            )
        )
    ]
    for copy in small:
        copy.start()
    barrier = pltpu.get_barrier_semaphore()
    for axis in range(3):
        for step in (1, 2, 3):
            pl.semaphore_signal(barrier, inc=1, device_id=peer(axis, step), device_id_type=MESH)
    head_copies = {}
    for k, pair in enumerate(PAIRS):
        span = pl.ds(FIRST_TILE[pair] * LANES, GROUPS[pair[0]][pair[1]] * LANES)
        head_copies[pair] = pltpu.make_async_copy(head_hbm.at[span], head_ref.at[span], head_sem.at[k])
        head_copies[pair].start()

    small[0].wait()
    small[1].wait()
    tiles = hidden_ref.shape[1] // LANES
    squares = jnp.zeros((16, LANES), jnp.float32)
    for k in range(tiles):
        part = hidden_ref[:, k * LANES : (k + 1) * LANES].astype(jnp.float32)
        squares += part * part
    scale = lax.rsqrt(jnp.sum(squares, axis=1, keepdims=True) / hidden_ref.shape[1] + EPSILON)
    for k in range(tiles):
        part = hidden_ref[:, k * LANES : (k + 1) * LANES].astype(jnp.float32)
        gain = gain_ref[:, k * LANES : (k + 1) * LANES].astype(jnp.float32)
        rows_ref[k, at[0], at[1], at[2]] = (part * scale * gain).astype(jnp.bfloat16)
    pl.semaphore_wait(barrier, 9)

    number = {m: k for k, m in enumerate(MESSAGES)}
    sent = []

    def message(p, g, phase, kind, taking):
        axis = ROUTES[p][phase]
        side = kind if kind < 2 else SIDES[p, g, phase]
        up = 1 if side == 0 else 3
        begun = (SIDE - up) * (2 if kind == 2 else 1) if taking else ((SIDE - up) if kind == 2 else 0)
        index = [pl.ds(FIRST_TILE[p, g], GROUPS[p][g]), *at]
        for done in range(phase):
            index[1 + ROUTES[p][done]] = pl.ds(0, SIDE)
        index[1 + axis] = lax.rem(at[axis] + begun, SIDE)
        block = rows_ref.at[tuple(index)]
        k = number[p, g, phase, kind]
        return pltpu.make_async_remote_copy(
            src_ref=block,
            dst_ref=block,
            send_sem=send_sem.at[k],
            recv_sem=take_sem.at[k],
            device_id=peer(axis, up),
            device_id_type=MESH,
        )

    def send(*key):
        copy = message(*key, False)
        copy.start()
        sent.append(copy)

    def multiply(p, g):
        first, many = FIRST_TILE[p, g], GROUPS[p][g]
        head_copies[p, g].wait()

        def strip(n, carry):
            columns = pl.ds(pl.multiple_of(n * 256, 256), 256)
            left = jnp.concatenate(
                [rows_ref[first + k].reshape(logits_ref.shape[0], LANES) for k in range(many)], axis=1
            )
            logits_ref[:, columns] += jnp.dot(
                left, head_ref[first * LANES : (first + many) * LANES, columns], preferred_element_type=jnp.float32
            )
            return carry

        lax.fori_loop(0, width // 256, strip, 0)

    def put(ref, stage, axis, values):
        for k, value in enumerate(values):
            ref[stage, at[axis], k] = value

    def swap(ref, stage, number_of, axis):
        copies = []
        for step in (1, 2, 3):
            block = ref.at[stage, at[axis]]
            copy = pltpu.make_async_remote_copy(
                src_ref=block,
                dst_ref=block,
                send_sem=swap_send_sem.at[number_of, step - 1],
                recv_sem=swap_take_sem.at[number_of, step - 1],
                device_id=peer(axis, step),
                device_id_type=MESH,
            )
            copy.start()
            copies.append(copy)
        sent.extend(copies)
        return copies

    def taken(ref, stage, number_of, axis):
        for step in (1, 2, 3):
            block = ref.at[stage, lax.rem(at[axis] + SIDE - step, SIDE)]
            pltpu.make_async_remote_copy(
                src_ref=block,
                dst_ref=block,
                send_sem=swap_send_sem.at[number_of, step - 1],
                recv_sem=swap_take_sem.at[number_of, step - 1],
                device_id=peer(axis, step),
                device_id_type=MESH,
            ).wait_recv()

    def joined_pair(stage):
        tops = [pair_ref[stage, c, 0] for c in range(SIDE)]
        top = jnp.maximum(jnp.maximum(tops[0], tops[1]), jnp.maximum(tops[2], tops[3]))
        total = sum(pair_ref[stage, c, 1] * jnp.exp(tops[c] - top) for c in range(SIDE))
        return top, total

    def summed(stage):
        return [sum(triple_ref[stage, c, k] for c in range(SIDE)) for k in range(3)]

    def rows_of(b):
        return pl.ds(pl.multiple_of(b * LANES, LANES), LANES)

    def stat_row(k, b):
        return stat_ref[k, pl.ds(b, 1), :]

    def set_stat(k, b, value):
        stat_ref[k, pl.ds(b, 1), :] = value

    def down(matrix, combine):
        return combine(jnp.transpose(matrix), axis=0, keepdims=True)

    lane = lax.broadcasted_iota(jnp.int32, (LANES, LANES), 1).astype(jnp.float32)

    def pickers(b):
        parent = as_column(parents_ref[pl.ds(b, 1), :].astype(jnp.float32))
        below = (lax.broadcasted_iota(jnp.int32, (LANES, LANES), 0) // NODES * NODES).astype(jnp.float32)
        hot = jnp.where(parent + below == lane, 1.0, 0.0).astype(jnp.bfloat16)
        token = as_column((tokens_ref[pl.ds(b, 1), :] - me * width).astype(jnp.float32))
        return hot, token

    def picked(pieces, hot, token):
        total = jnp.zeros((LANES, LANES), jnp.float32)
        for c in range(width // 256):
            found = sum(
                jnp.dot(hot, piece, preferred_element_type=jnp.float32)
                for piece in pieces(slice(c * 256, (c + 1) * 256))
            )
            for half in range(2):
                here = found[:, half * LANES : (half + 1) * LANES]
                total += jnp.where(token == lane + float(c * 256 + half * LANES), here, 0.0)
        return total

    def column_tiles():
        return [slice(c * LANES, (c + 1) * LANES) for c in range(width // LANES)]

    def draft_stats(b, carry):
        rows = rows_of(b)
        top = jnp.full((LANES, LANES), -jnp.inf, jnp.float32)
        for tile in column_tiles():
            top = jnp.maximum(top, draft_ref[rows, tile].astype(jnp.float32))
        top = down(top, jnp.max)
        column = as_column(top)
        total = jnp.zeros((LANES, LANES), jnp.float32)
        for tile in column_tiles():
            total += jnp.exp(draft_ref[rows, tile].astype(jnp.float32) - column)
        set_stat(0, b, top)
        set_stat(1, b, down(total, jnp.sum))
        hot, token = pickers(b)
        set_stat(2, b, down(picked(lambda tile: [draft_ref[rows, tile]], hot, token), jnp.sum))
        return carry

    def draft_probs(b, carry):
        rows = rows_of(b)
        column = as_column(stat_row(6, b))
        for tile in column_tiles():
            draft_prob_ref[rows, tile] = jnp.exp(draft_ref[rows, tile].astype(jnp.float32) - column)
        return carry

    def target_stats(b, carry):
        rows = rows_of(b)
        top = jnp.full((LANES, LANES), -jnp.inf, jnp.float32)
        for tile in column_tiles():
            top = jnp.maximum(top, logits_ref[rows, tile])
        top = down(top, jnp.max)
        column = as_column(top)
        total = jnp.zeros((LANES, LANES), jnp.float32)
        for tile in column_tiles():
            weight = jnp.exp(logits_ref[rows, tile] - column)
            weight_ref[rows, tile] = weight
            total += weight
        set_stat(3, b, top)
        set_stat(4, b, down(total, jnp.sum))
        return carry

    def target_picks(b, carry):
        rows = rows_of(b)

        def pieces(tile):
            values = logits_ref[rows, tile]
            high = values.astype(jnp.bfloat16)
            rest = values - high.astype(jnp.float32)
            middle = rest.astype(jnp.bfloat16)
            low = (rest - middle.astype(jnp.float32)).astype(jnp.bfloat16)
            return high, middle, low

        hot, token = pickers(b)
        set_stat(5, b, down(picked(pieces, hot, token), jnp.sum))
        return carry

    def residuals(b, carry):
        rows = rows_of(b)
        factor = as_column(stat_row(7, b))
        total = jnp.zeros((LANES, LANES), jnp.float32)
        for tile in column_tiles():
            total += jnp.maximum(weight_ref[rows, tile] * factor - draft_prob_ref[rows, tile], 0.0)
        set_stat(8, b, down(total, jnp.sum))
        return carry

    def over(body, low=0, high=spans):
        lax.fori_loop(low, high, body, 0)

    def draft_work():
        for c in (2, 3, 4):
            small[c].wait()
        yield
        for b in range(0, spans, 2):
            over(draft_stats, b, b + 2)
            yield
        put(pair_ref, 0, 0, (stat_ref[0], stat_ref[1]))
        yield
        swap(pair_ref, 0, 0, 0)
        yield
        for axis in (1, 2):
            yield
            yield
            taken(pair_ref, axis - 1, axis - 1, axis - 1)
            put(pair_ref, axis, axis, joined_pair(axis - 1))
            yield
            swap(pair_ref, axis, axis, axis)
            yield
        yield
        yield
        taken(pair_ref, 2, 2, 2)
        top, total = joined_pair(2)
        stat_ref[6] = top + jnp.log(total)
        for b in range(0, spans, 4):
            yield
            over(draft_probs, b, b + 4)

    for g in range(max(map(len, GROUPS))):
        for p in range(3):
            if g < len(GROUPS[p]):
                send(p, g, 0, 0)
                send(p, g, 0, 1)
    def clear(b, carry):
        logits_ref[rows_of(b)] = jnp.zeros((LANES, width), jnp.float32)
        return carry

    over(clear)
    have = set()
    draft = draft_work()
    for step, (kind, key) in enumerate(ORDER):
        if kind == "multiply":
            multiply(*key)
            continue
        message(*key, True).wait_recv()
        p, g, phase, way = key
        have.add(key)
        if way == SIDES[p, g, phase]:
            send(p, g, phase, 2)
        if phase < 2 and all((p, g, phase, k) in have for k in range(3)):
            send(p, g, phase + 1, 0)
            send(p, g, phase + 1, 1)
        if step >= 24 and step % 3 == 0:
            next(draft, None)
    for _ in draft:
        pass

    over(target_stats)
    put(pair_ref, 3, 0, (stat_ref[3], stat_ref[4]))
    swap(pair_ref, 3, 3, 0)
    over(target_picks, 0, spans // 2)
    taken(pair_ref, 3, 3, 0)
    put(pair_ref, 4, 1, joined_pair(3))
    swap(pair_ref, 4, 4, 1)
    over(target_picks, spans // 2, spans)
    taken(pair_ref, 4, 4, 1)
    put(pair_ref, 5, 2, joined_pair(4))
    swap(pair_ref, 5, 5, 2)
    taken(pair_ref, 5, 5, 2)
    top, total = joined_pair(5)
    target_lse = top + jnp.log(total)
    stat_ref[7] = jnp.exp(stat_ref[3] - target_lse)
    over(residuals)
    values = (stat_ref[8], stat_ref[5], stat_ref[2])
    for axis in range(3):
        put(triple_ref, axis, axis, values)
        swap(triple_ref, axis, 6 + axis, axis)
        taken(triple_ref, axis, 6 + axis, axis)
        values = summed(axis)
    out_ref[0] = target_lse
    out_ref[1] = stat_ref[6]
    for k in range(3):
        out_ref[2 + k] = values[k]
    for copy in sent:
        copy.wait_send()


def tree_kernel(stats_ref, parents_ref, depths_ref, uniforms_ref, lse_ref, token_ref, residual_ref, accept_ref, path_ref):
    lanes = lax.broadcasted_iota(jnp.int32, parents_ref.shape, 1)
    parent = lanes // NODES * NODES + parents_ref[...]

    def at_parent(vector):
        return jnp.take_along_axis(vector, parent, axis=1)

    target_lse = stats_ref[0]
    token_logprob = stats_ref[3] - at_parent(target_lse)
    draft_logprob = stats_ref[4] - at_parent(stats_ref[1])
    accept = jnp.exp(jnp.minimum(token_logprob - draft_logprob, 0.0)) - uniforms_ref[...]
    depths = depths_ref[...]
    path = jnp.ones(accept.shape, jnp.float32)
    for level in range(1, DEPTH_MAX + 1):
        path = jnp.where(depths == level, jnp.minimum(accept, at_parent(path)), path)
    lse_ref[...] = target_lse
    token_ref[...] = token_logprob
    residual_ref[...] = stats_ref[2]
    accept_ref[...] = accept
    path_ref[...] = path


def body(hidden, norm_gain, lm_head, draft_logits, draft_tokens, tree_parents, node_depths, uniforms):
    depth, width = lm_head.shape
    rows = draft_logits.shape[0]
    spans = rows // LANES
    flat = (spans, LANES)
    hbm = pl.BlockSpec(memory_space=pltpu.HBM)
    vmem = pl.BlockSpec(memory_space=pltpu.VMEM)
    stats = pl.pallas_call(
        main_kernel,
        out_shape=jax.ShapeDtypeStruct((5, *flat), jnp.float32),
        in_specs=[hbm] * 6,
        out_specs=vmem,
        scratch_shapes=[
            pltpu.VMEM(hidden.shape, jnp.bfloat16),
            pltpu.VMEM((1, depth), jnp.bfloat16),
            pltpu.VMEM((depth, width), jnp.bfloat16),
            pltpu.VMEM((rows, width), jnp.bfloat16),
            pltpu.VMEM(flat, jnp.int32),
            pltpu.VMEM(flat, jnp.int32),
            pltpu.VMEM((depth // LANES, SIDE, SIDE, SIDE, hidden.shape[0], LANES), jnp.bfloat16),
            pltpu.VMEM((rows, width), jnp.float32),
            pltpu.VMEM((rows, width), jnp.float32),
            pltpu.VMEM((rows, width), jnp.float32),
            pltpu.VMEM((9, *flat), jnp.float32),
            pltpu.VMEM((6, SIDE, 2, *flat), jnp.float32),
            pltpu.VMEM((3, SIDE, 3, *flat), jnp.float32),
            pltpu.SemaphoreType.DMA((5,)),
            pltpu.SemaphoreType.DMA((len(PAIRS),)),
            pltpu.SemaphoreType.DMA((len(MESSAGES),)),
            pltpu.SemaphoreType.DMA((len(MESSAGES),)),
            pltpu.SemaphoreType.DMA((9, 3)),
            pltpu.SemaphoreType.DMA((9, 3)),
        ],
        compiler_params=pltpu.CompilerParams(
            collective_id=0, has_side_effects=True, vmem_limit_bytes=60 * 2**20
        ),
        name="gather_verify",
    )(
        hidden,
        norm_gain.reshape(1, depth),
        lm_head,
        draft_logits,
        draft_tokens.reshape(flat),
        tree_parents.reshape(flat),
    )
    outs = pl.pallas_call(
        tree_kernel,
        out_shape=[jax.ShapeDtypeStruct(flat, jnp.float32)] * 5,
        in_specs=[vmem] * 4,
        out_specs=[vmem] * 5,
        name="tree",
    )(stats, tree_parents.reshape(flat), node_depths.reshape(flat), uniforms.reshape(flat))
    return tuple(out.reshape(rows) for out in outs)


def solution(mesh):
    return jax.shard_map(
        body,
        mesh=mesh,
        in_specs=(
            P(("batch", "vocab"), None),
            P(),
            P(None, "vocab"),
            P("batch", "vocab"),
            P("batch"),
            P("batch"),
            P("batch"),
            P("batch"),
        ),
        out_specs=(P("batch"), P("batch"), P("batch"), P("batch"), P("batch")),
        check_vma=False,
    )
```

```python
import heapq
import itertools

import jax
import jax.numpy as jnp
from jax import lax
from jax.experimental import pallas as pl
from jax.experimental.pallas import tpu as pltpu
from jax.sharding import PartitionSpec as P

NODES = 64
DEPTH_MAX = 8
EPSILON = 1e-06
LANES = 128
SIDE = 4
MESH = pl.DeviceIdType.MESH

ROUTES = ((0, 1, 2), (1, 2, 0), (2, 0, 1))
GROUPS = ((2, 4, 4, 4, 4, 1), (2, 4, 4, 4, 4, 1), (2, 4, 4, 4, 3, 1))


def relay_sides():
    sides = {}
    for p, sizes in enumerate(GROUPS):
        for phase in range(3):
            lean = 0
            for g in sorted(range(len(sizes)), key=lambda g: -sizes[g]):
                sides[p, g, phase] = 0 if lean <= 0 else 1
                lean += sizes[g] if lean <= 0 else -sizes[g]
    return sides


SIDES = relay_sides()


DRAFT = (
    [(("stats", b), 0.45, 2.0 if b == 0 else 0.0) for b in range(8)]
    + [(("join", axis), 0.3, 12.0 if axis else 0.0) for axis in range(4)]
    + [(("probs", b), 0.2, 0.0) for b in range(8)]
)
STRIPS = 2


def plan():
    rate, gap, latency = 44500.0, 0.2, 2.5
    free = {(a, d): 0.0 for a in range(3) for d in range(2)}
    coming, count, have, order, ready = [], itertools.count(), set(), [], []
    draft = list(DRAFT)

    def send(now, p, g, phase, kind):
        way = (ROUTES[p][phase], kind if kind < 2 else SIDES[p, g, phase])
        free[way] = max(now, free[way]) + gap + GROUPS[p][g] * 4096 * SIDE**phase / rate
        heapq.heappush(coming, (free[way] + latency, next(count), (p, g, phase, kind)))

    now, last = 0.0, 0.0
    for g in range(max(map(len, GROUPS))):
        for p in range(3):
            if g < len(GROUPS[p]):
                send(now, p, g, 0, 0)
                send(now, p, g, 0, 1)
    while coming or ready or draft:
        due = last + draft[0][2] if draft else float("inf")
        if coming and coming[0][0] <= now or not ready and coming and coming[0][0] <= due:
            at, _, message = heapq.heappop(coming)
            now = max(now, at) + 0.05
            p, g, phase, kind = message
            have.add(message)
            order.append(("take", message))
            if kind == SIDES[p, g, phase]:
                send(now, p, g, phase, 2)
            if all((p, g, phase, k) in have for k in range(3)):
                if phase < 2:
                    send(now, p, g, phase + 1, 0)
                    send(now, p, g, phase + 1, 1)
                else:
                    ready.extend((p, g, n) for n in range(STRIPS))
        elif draft and (due <= now or not ready):
            what, cost, _ = draft.pop(0)
            order.append(("draft", what))
            now = last = max(now, due) + cost
        else:
            p, g, n = ready.pop(0)
            order.append(("multiply", (p, g, n)))
            now += 0.05 + 0.32 / STRIPS * max(2, GROUPS[p][g])
    return order


ORDER = plan()
PAIRS = [key[:2] for kind, key in ORDER if kind == "multiply" and key[2] == 0]
MESSAGES = [m for kind, m in ORDER if kind == "take"]
FIRST_TILE = {
    (p, g): sum(map(sum, GROUPS[:p])) + sum(GROUPS[p][:g]) for p in range(3) for g in range(len(GROUPS[p]))
}


def as_column(row):
    return jnp.transpose(jnp.broadcast_to(row, (LANES, LANES)))


def main_kernel(
    hidden_hbm, gain_hbm, head_hbm, draft_hbm, tokens_hbm, parents_hbm,
    out_ref,
    hidden_ref, gain_ref, head_ref, draft_ref, tokens_ref, parents_ref,
    rows_ref, logits_ref, weight_ref, draft_prob_ref, stat_ref, pair_ref, bank_ref,
    small_sem, head_sem, send_sem, take_sem, swap_send_sem, swap_take_sem, far_send_sem, far_take_sem,
):
    me = lax.axis_index("vocab")
    batch = lax.axis_index("batch")
    at = (me // 16, (me // 4) % 4, me % 4)
    stride = (16, 4, 1)
    width = logits_ref.shape[1]
    spans = logits_ref.shape[0] // LANES

    def peer(axis, step):
        return (me + (lax.rem(at[axis] + step, SIDE) - at[axis]) * stride[axis], batch)

    small = [
        pltpu.make_async_copy(src, dst, small_sem.at[k])
        for k, (src, dst) in enumerate(
            (
                (hidden_hbm, hidden_ref),
                (gain_hbm, gain_ref),
                (draft_hbm, draft_ref),
                (tokens_hbm, tokens_ref),
                (parents_hbm, parents_ref),
            )
        )
    ]
    for copy in small:
        copy.start()
    barrier = pltpu.get_barrier_semaphore()
    for axis in range(3):
        for step in (1, 2, 3):
            pl.semaphore_signal(barrier, inc=1, device_id=peer(axis, step), device_id_type=MESH)
    head_copies = {}
    for k, pair in enumerate(PAIRS):
        span = pl.ds(FIRST_TILE[pair] * LANES, GROUPS[pair[0]][pair[1]] * LANES)
        head_copies[pair] = pltpu.make_async_copy(head_hbm.at[span], head_ref.at[span], head_sem.at[k])
        head_copies[pair].start()

    small[0].wait()
    small[1].wait()
    tiles = hidden_ref.shape[1] // LANES
    squares = jnp.zeros((16, LANES), jnp.float32)
    for k in range(tiles):
        part = hidden_ref[:, k * LANES : (k + 1) * LANES].astype(jnp.float32)
        squares += part * part
    scale = lax.rsqrt(jnp.sum(squares, axis=1, keepdims=True) / hidden_ref.shape[1] + EPSILON)
    for k in range(tiles):
        part = hidden_ref[:, k * LANES : (k + 1) * LANES].astype(jnp.float32)
        gain = gain_ref[k : k + 1, :].astype(jnp.float32)
        rows_ref[k, at[0], at[1], at[2]] = (part * scale * gain).astype(jnp.bfloat16)
    pl.semaphore_wait(barrier, 9)

    number = {m: k for k, m in enumerate(MESSAGES)}
    sent = []

    def message(p, g, phase, kind, taking):
        axis = ROUTES[p][phase]
        side = kind if kind < 2 else SIDES[p, g, phase]
        up = 1 if side == 0 else 3
        begun = (SIDE - up) * (2 if kind == 2 else 1) if taking else ((SIDE - up) if kind == 2 else 0)
        index = [pl.ds(FIRST_TILE[p, g], GROUPS[p][g]), *at]
        for done in range(phase):
            index[1 + ROUTES[p][done]] = pl.ds(0, SIDE)
        index[1 + axis] = lax.rem(at[axis] + begun, SIDE)
        block = rows_ref.at[tuple(index)]
        k = number[p, g, phase, kind]
        return pltpu.make_async_remote_copy(
            src_ref=block,
            dst_ref=block,
            send_sem=send_sem.at[k],
            recv_sem=take_sem.at[k],
            device_id=peer(axis, up),
            device_id_type=MESH,
        )

    def send(*key):
        copy = message(*key, False)
        copy.start()
        sent.append(copy)

    def multiply(p, g, n):
        first, many = FIRST_TILE[p, g], GROUPS[p][g]
        if n == 0:
            head_copies[p, g].wait()
        columns = slice(n * width // STRIPS, (n + 1) * width // STRIPS)
        left = jnp.concatenate(
            [rows_ref[first + k].reshape(logits_ref.shape[0], LANES) for k in range(many)], axis=1
        )
        product = jnp.dot(
            left, head_ref[first * LANES : (first + many) * LANES, columns], preferred_element_type=jnp.float32
        )
        if (p, g) == PAIRS[0]:
            logits_ref[:, columns] = product
        else:
            logits_ref[:, columns] += product

    def put(ref, stage, axis, values):
        for k, value in enumerate(values):
            ref[stage, at[axis], k] = value

    def swap(ref, stage, number_of, axis):
        copies = []
        for step in (1, 2, 3):
            block = ref.at[stage, at[axis]]
            copy = pltpu.make_async_remote_copy(
                src_ref=block,
                dst_ref=block,
                send_sem=swap_send_sem.at[number_of, step - 1],
                recv_sem=swap_take_sem.at[number_of, step - 1],
                device_id=peer(axis, step),
                device_id_type=MESH,
            )
            copy.start()
            copies.append(copy)
        sent.extend(copies)
        return copies

    def taken(ref, stage, number_of, axis):
        for step in (1, 2, 3):
            block = ref.at[stage, lax.rem(at[axis] + SIDE - step, SIDE)]
            pltpu.make_async_remote_copy(
                src_ref=block,
                dst_ref=block,
                send_sem=swap_send_sem.at[number_of, step - 1],
                recv_sem=swap_take_sem.at[number_of, step - 1],
                device_id=peer(axis, step),
                device_id_type=MESH,
            ).wait_recv()

    def joined_pair(stage):
        tops = [pair_ref[stage, c, 0] for c in range(SIDE)]
        top = jnp.maximum(jnp.maximum(tops[0], tops[1]), jnp.maximum(tops[2], tops[3]))
        total = sum(pair_ref[stage, c, 1] * jnp.exp(tops[c] - top) for c in range(SIDE))
        return top, total, sum(pair_ref[stage, c, 2] for c in range(SIDE))

    shifts = sorted(
        (o for o in itertools.product(range(SIDE), repeat=3) if any(o)), key=lambda o: -sum(min(v, SIDE - v) for v in o)
    )

    def across(turn, k, back):
        there = me
        for axis in range(3):
            step = shifts[k][axis]
            here = lax.rem(at[axis] + (SIDE - step if back else step), SIDE)
            there = there + (here - at[axis]) * stride[axis]
        block = bank_ref.at[turn, there if back else me]
        return pltpu.make_async_remote_copy(
            src_ref=block,
            dst_ref=block,
            send_sem=far_send_sem.at[turn, k],
            recv_sem=far_take_sem.at[turn, k],
            device_id=(there, batch),
            device_id_type=MESH,
        )

    def cast(turn, value):
        bank_ref[turn, me] = value
        for k in range(len(shifts)):
            copy = across(turn, k, False)
            copy.start()
            sent.append(copy)

    def collected(turn):
        for k in range(len(shifts)):
            across(turn, k, True).wait_recv()
        return [bank_ref[turn, v] for v in range(len(shifts) + 1)]

    def joined_lse(values):
        top = values[0]
        for value in values[1:]:
            top = jnp.maximum(top, value)
        return top + jnp.log(sum(jnp.exp(value - top) for value in values))

    def rows_of(b):
        return pl.ds(pl.multiple_of(b * LANES, LANES), LANES)

    def stat_row(k, b):
        return stat_ref[k, pl.ds(b, 1), :]

    def set_stat(k, b, value):
        stat_ref[k, pl.ds(b, 1), :] = value

    def down(matrix, combine):
        return combine(jnp.transpose(matrix), axis=0, keepdims=True)

    lane = lax.broadcasted_iota(jnp.int32, (LANES, LANES), 1).astype(jnp.float32)

    def pickers(b):
        parent = as_column(parents_ref[pl.ds(b, 1), :].astype(jnp.float32))
        below = (lax.broadcasted_iota(jnp.int32, (LANES, LANES), 0) // NODES * NODES).astype(jnp.float32)
        hot = jnp.where(parent + below == lane, 1.0, 0.0).astype(jnp.bfloat16)
        token = as_column((tokens_ref[pl.ds(b, 1), :] - me * width).astype(jnp.float32))
        return hot, token

    def picked(pieces, hot, token):
        total = jnp.zeros((LANES, LANES), jnp.float32)
        for c in range(width // 256):
            found = sum(
                jnp.dot(hot, piece, preferred_element_type=jnp.float32)
                for piece in pieces(slice(c * 256, (c + 1) * 256))
            )
            for half in range(2):
                here = found[:, half * LANES : (half + 1) * LANES]
                total += jnp.where(token == lane + float(c * 256 + half * LANES), here, 0.0)
        return total

    def column_tiles():
        return [slice(c * LANES, (c + 1) * LANES) for c in range(width // LANES)]

    def draft_stats(b, carry):
        rows = rows_of(b)
        top = jnp.full((LANES, LANES), -jnp.inf, jnp.float32)
        for tile in column_tiles():
            top = jnp.maximum(top, draft_ref[rows, tile].astype(jnp.float32))
        top = down(top, jnp.max)
        column = as_column(top)
        total = jnp.zeros((LANES, LANES), jnp.float32)
        for tile in column_tiles():
            total += jnp.exp(draft_ref[rows, tile].astype(jnp.float32) - column)
        set_stat(0, b, top)
        set_stat(1, b, down(total, jnp.sum))
        hot, token = pickers(b)
        set_stat(2, b, down(picked(lambda tile: [draft_ref[rows, tile]], hot, token), jnp.sum))
        return carry

    def draft_probs(b, carry):
        rows = rows_of(b)
        column = as_column(stat_row(6, b))
        for tile in column_tiles():
            draft_prob_ref[rows, tile] = jnp.exp(draft_ref[rows, tile].astype(jnp.float32) - column)
        return carry

    def target_stats(b, carry):
        rows = rows_of(b)
        top = jnp.full((LANES, LANES), -jnp.inf, jnp.float32)
        for tile in column_tiles():
            top = jnp.maximum(top, logits_ref[rows, tile])
        top = down(top, jnp.max)
        column = as_column(top)
        total = jnp.zeros((LANES, LANES), jnp.float32)
        for tile in column_tiles():
            weight = jnp.exp(logits_ref[rows, tile] - column)
            weight_ref[rows, tile] = weight
            total += weight
        set_stat(3, b, top)
        set_stat(4, b, down(total, jnp.sum))
        return carry

    def target_picks(b, carry):
        rows = rows_of(b)

        def pieces(tile):
            values = logits_ref[rows, tile]
            high = values.astype(jnp.bfloat16)
            rest = values - high.astype(jnp.float32)
            middle = rest.astype(jnp.bfloat16)
            low = (rest - middle.astype(jnp.float32)).astype(jnp.bfloat16)
            return high, middle, low

        hot, token = pickers(b)
        set_stat(5, b, down(picked(pieces, hot, token), jnp.sum))
        return carry

    def residuals(b, carry):
        rows = rows_of(b)
        factor = as_column(stat_row(7, b))
        total = jnp.zeros((LANES, LANES), jnp.float32)
        for tile in column_tiles():
            total += jnp.maximum(weight_ref[rows, tile] * factor - draft_prob_ref[rows, tile], 0.0)
        set_stat(8, b, down(total, jnp.sum))
        return carry

    def over(body, unroll):
        lax.fori_loop(0, spans, body, 0, unroll=unroll)

    def work_on_draft(what, which):
        if what == "stats":
            if which == 0:
                for copy in small[2:]:
                    copy.wait()
            draft_stats(which, 0)
        elif what == "probs":
            draft_probs(which, 0)
        else:
            if which:
                taken(pair_ref, which - 1, which - 1, which - 1)
            values = joined_pair(which - 1) if which else (stat_ref[0], stat_ref[1], stat_ref[2])
            if which < 3:
                put(pair_ref, which, which, values)
                swap(pair_ref, which, which, which)
            else:
                stat_ref[6] = values[0] + jnp.log(values[1])
                out_ref[1] = stat_ref[6]
                out_ref[4] = values[2]

    for g in range(max(map(len, GROUPS))):
        for p in range(3):
            if g < len(GROUPS[p]):
                send(p, g, 0, 0)
                send(p, g, 0, 1)
    have = set()
    for kind, key in ORDER:
        if kind == "multiply":
            multiply(*key)
        elif kind == "draft":
            work_on_draft(*key)
        else:
            message(*key, True).wait_recv()
            p, g, phase, way = key
            have.add(key)
            if way == SIDES[p, g, phase]:
                send(p, g, phase, 2)
            if phase < 2 and all((p, g, phase, k) in have for k in range(3)):
                send(p, g, phase + 1, 0)
                send(p, g, phase + 1, 1)

    over(target_stats, spans)
    cast(0, stat_ref[3] + jnp.log(stat_ref[4]))
    over(target_picks, 2)
    cast(1, stat_ref[5])
    target_lse = joined_lse(collected(0))
    stat_ref[7] = jnp.exp(stat_ref[3] - target_lse)
    over(residuals, spans)
    cast(2, stat_ref[8])
    out_ref[0] = target_lse
    out_ref[3] = sum(collected(1))
    out_ref[2] = sum(collected(2))
    for copy in sent:
        copy.wait_send()


def tree_kernel(stats_ref, parents_ref, depths_ref, uniforms_ref, lse_ref, token_ref, residual_ref, accept_ref, path_ref):
    lanes = lax.broadcasted_iota(jnp.int32, parents_ref.shape, 1)
    parent = lanes // NODES * NODES + parents_ref[...]

    def at_parent(vector):
        return jnp.take_along_axis(vector, parent, axis=1)

    target_lse = stats_ref[0]
    token_logprob = stats_ref[3] - at_parent(target_lse)
    draft_logprob = stats_ref[4] - at_parent(stats_ref[1])
    accept = jnp.exp(jnp.minimum(token_logprob - draft_logprob, 0.0)) - uniforms_ref[...]
    depths = depths_ref[...]
    path = jnp.ones(accept.shape, jnp.float32)
    for level in range(1, DEPTH_MAX + 1):
        path = jnp.where(depths == level, jnp.minimum(accept, at_parent(path)), path)
    lse_ref[...] = target_lse
    token_ref[...] = token_logprob
    residual_ref[...] = stats_ref[2]
    accept_ref[...] = accept
    path_ref[...] = path


def body(hidden, norm_gain, lm_head, draft_logits, draft_tokens, tree_parents, node_depths, uniforms):
    depth, width = lm_head.shape
    rows = draft_logits.shape[0]
    spans = rows // LANES
    flat = (spans, LANES)
    hbm = pl.BlockSpec(memory_space=pltpu.HBM)
    vmem = pl.BlockSpec(memory_space=pltpu.VMEM)
    stats = pl.pallas_call(
        main_kernel,
        out_shape=jax.ShapeDtypeStruct((5, *flat), jnp.float32),
        in_specs=[hbm] * 6,
        out_specs=vmem,
        scratch_shapes=[
            pltpu.VMEM(hidden.shape, jnp.bfloat16),
            pltpu.VMEM((depth // LANES, LANES), jnp.bfloat16),
            pltpu.VMEM((depth, width), jnp.bfloat16),
            pltpu.VMEM((rows, width), jnp.bfloat16),
            pltpu.VMEM(flat, jnp.int32),
            pltpu.VMEM(flat, jnp.int32),
            pltpu.VMEM((depth // LANES, SIDE, SIDE, SIDE, hidden.shape[0], LANES), jnp.bfloat16),
            pltpu.VMEM((rows, width), jnp.float32),
            pltpu.VMEM((rows, width), jnp.float32),
            pltpu.VMEM((rows, width), jnp.float32),
            pltpu.VMEM((9, *flat), jnp.float32),
            pltpu.VMEM((3, SIDE, 3, *flat), jnp.float32),
            pltpu.VMEM((3, SIDE**3, *flat), jnp.float32),
            pltpu.SemaphoreType.DMA((5,)),
            pltpu.SemaphoreType.DMA((len(PAIRS),)),
            pltpu.SemaphoreType.DMA((len(MESSAGES),)),
            pltpu.SemaphoreType.DMA((len(MESSAGES),)),
            pltpu.SemaphoreType.DMA((3, 3)),
            pltpu.SemaphoreType.DMA((3, 3)),
            pltpu.SemaphoreType.DMA((3, SIDE**3 - 1)),
            pltpu.SemaphoreType.DMA((3, SIDE**3 - 1)),
        ],
        compiler_params=pltpu.CompilerParams(
            collective_id=0, has_side_effects=True, vmem_limit_bytes=60 * 2**20
        ),
        name="gather_verify",
    )(
        hidden,
        norm_gain.reshape(depth // LANES, LANES),
        lm_head,
        draft_logits,
        draft_tokens.reshape(flat),
        tree_parents.reshape(flat),
    )
    outs = pl.pallas_call(
        tree_kernel,
        out_shape=[jax.ShapeDtypeStruct(flat, jnp.float32)] * 5,
        in_specs=[vmem] * 4,
        out_specs=[vmem] * 5,
        name="tree",
    )(stats, tree_parents.reshape(flat), node_depths.reshape(flat), uniforms.reshape(flat))
    return tuple(out.reshape(rows) for out in outs)


def solution(mesh):
    return jax.shard_map(
        body,
        mesh=mesh,
        in_specs=(
            P(("batch", "vocab"), None),
            P(),
            P(None, "vocab"),
            P("batch", "vocab"),
            P("batch"),
            P("batch"),
            P("batch"),
            P("batch"),
        ),
        out_specs=(P("batch"), P("batch"), P("batch"), P("batch"), P("batch")),
        check_vma=False,
    )
```

```python
import heapq
import itertools

import jax
import jax.numpy as jnp
from jax import lax
from jax.experimental import pallas as pl
from jax.experimental.pallas import tpu as pltpu
from jax.sharding import PartitionSpec as P

NODES = 64
DEPTH_MAX = 8
EPSILON = 1e-06
LANES = 128
SIDE = 4
MESH = pl.DeviceIdType.MESH

ROUTES = ((0, 1, 2), (1, 2, 0), (2, 0, 1))
GROUPS = ((2, 5, 6, 4, 2), (2, 5, 6, 4, 2), (2, 5, 6, 3, 2))


def relay_sides():
    sides = {}
    for p, sizes in enumerate(GROUPS):
        for phase in range(3):
            lean = 0
            for g in sorted(range(len(sizes)), key=lambda g: -sizes[g]):
                sides[p, g, phase] = 0 if lean <= 0 else 1
                lean += sizes[g] if lean <= 0 else -sizes[g]
    return sides


SIDES = relay_sides()


DRAFT = (
    [(("stats", b), 0.45, 2.0 if b == 0 else 0.0) for b in range(8)]
    + [(("join", axis), 0.3, 12.0 if axis else 0.0) for axis in range(4)]
    + [(("probs", b), 0.2, 0.0) for b in range(8)]
)


def plan():
    rate, gap, latency = 44500.0, 0.2, 2.5
    free = {(a, d): 0.0 for a in range(3) for d in range(2)}
    coming, count, have, order, ready = [], itertools.count(), set(), [], []
    draft = list(DRAFT)

    def send(now, p, g, phase, kind):
        way = (ROUTES[p][phase], kind if kind < 2 else SIDES[p, g, phase])
        free[way] = max(now, free[way]) + gap + GROUPS[p][g] * 4096 * SIDE**phase / rate
        heapq.heappush(coming, (free[way] + latency, next(count), (p, g, phase, kind)))

    now, last = 0.0, 0.0
    for g in range(max(map(len, GROUPS))):
        for p in range(3):
            if g < len(GROUPS[p]):
                send(now, p, g, 0, 0)
                send(now, p, g, 0, 1)
    while coming or ready or draft:
        due = last + draft[0][2] if draft else float("inf")
        if coming and coming[0][0] <= now or not ready and coming and coming[0][0] <= due:
            at, _, message = heapq.heappop(coming)
            now = max(now, at) + 0.05
            p, g, phase, kind = message
            have.add(message)
            order.append(("take", message))
            if kind == SIDES[p, g, phase]:
                send(now, p, g, phase, 2)
            if all((p, g, phase, k) in have for k in range(3)):
                if phase < 2:
                    send(now, p, g, phase + 1, 0)
                    send(now, p, g, phase + 1, 1)
                if phase == 1:
                    ready.append((p, g, 3))
            if phase == 2:
                ready.append((p, g, kind))
        elif draft and (due <= now or not ready):
            what, cost, _ = draft.pop(0)
            order.append(("draft", what))
            now = last = max(now, due) + cost
        else:
            p, g, kind = ready.pop(0)
            order.append(("multiply", (p, g, kind)))
            now += 0.2 + 0.08 * max(2, GROUPS[p][g])
    return order


ORDER = plan()
PAIRS = [key[:2] for kind, key in ORDER if kind == "multiply" and key[2] == 3]
MESSAGES = [m for kind, m in ORDER if kind == "take"]
FIRST_TILE = {
    (p, g): sum(map(sum, GROUPS[:p])) + sum(GROUPS[p][:g]) for p in range(3) for g in range(len(GROUPS[p]))
}


def as_column(row):
    return jnp.transpose(jnp.broadcast_to(row, (LANES, LANES)))


def main_kernel(
    hidden_hbm, gain_hbm, head_hbm, draft_hbm, tokens_hbm, parents_hbm,
    out_ref,
    hidden_ref, gain_ref, head_ref, draft_ref, tokens_ref, parents_ref,
    rows_ref, logits_ref, weight_ref, draft_prob_ref, stat_ref, pair_ref, bank_ref,
    small_sem, head_sem, send_sem, take_sem, swap_send_sem, swap_take_sem, far_send_sem, far_take_sem,
):
    me = lax.axis_index("vocab")
    batch = lax.axis_index("batch")
    at = (me // 16, (me // 4) % 4, me % 4)
    stride = (16, 4, 1)
    width = weight_ref.shape[1]
    spans = weight_ref.shape[0] // LANES

    def peer(axis, step):
        return (me + (lax.rem(at[axis] + step, SIDE) - at[axis]) * stride[axis], batch)

    small = [
        pltpu.make_async_copy(src, dst, small_sem.at[k])
        for k, (src, dst) in enumerate(
            (
                (hidden_hbm, hidden_ref),
                (gain_hbm, gain_ref),
                (draft_hbm, draft_ref),
                (tokens_hbm, tokens_ref),
                (parents_hbm, parents_ref),
            )
        )
    ]
    for copy in small:
        copy.start()
    barrier = pltpu.get_barrier_semaphore()
    for axis in range(3):
        for step in (1, 2, 3):
            pl.semaphore_signal(barrier, inc=1, device_id=peer(axis, step), device_id_type=MESH)
    head_copies = {}
    for k, pair in enumerate(PAIRS):
        span = pl.ds(FIRST_TILE[pair] * LANES, GROUPS[pair[0]][pair[1]] * LANES)
        head_copies[pair] = pltpu.make_async_copy(head_hbm.at[span], head_ref.at[span], head_sem.at[k])
        head_copies[pair].start()

    small[0].wait()
    small[1].wait()
    tiles = hidden_ref.shape[1] // LANES
    squares = jnp.zeros((16, LANES), jnp.float32)
    for k in range(tiles):
        part = hidden_ref[:, k * LANES : (k + 1) * LANES].astype(jnp.float32)
        squares += part * part
    scale = lax.rsqrt(jnp.sum(squares, axis=1, keepdims=True) / hidden_ref.shape[1] + EPSILON)
    for k in range(tiles):
        part = hidden_ref[:, k * LANES : (k + 1) * LANES].astype(jnp.float32)
        gain = gain_ref[k : k + 1, :].astype(jnp.float32)
        rows_ref[k, at[0], at[1], at[2]] = (part * scale * gain).astype(jnp.bfloat16)
    for y in range(SIDE):
        logits_ref[y] = jnp.zeros(logits_ref.shape[1:], jnp.float32)
    pl.semaphore_wait(barrier, 9)

    number = {m: k for k, m in enumerate(MESSAGES)}
    sent = []

    def message(p, g, phase, kind, taking):
        axis = ROUTES[p][phase]
        side = kind if kind < 2 else SIDES[p, g, phase]
        up = 1 if side == 0 else 3
        begun = (SIDE - up) * (2 if kind == 2 else 1) if taking else ((SIDE - up) if kind == 2 else 0)
        index = [pl.ds(FIRST_TILE[p, g], GROUPS[p][g]), *at]
        for done in range(phase):
            index[1 + ROUTES[p][done]] = pl.ds(0, SIDE)
        index[1 + axis] = lax.rem(at[axis] + begun, SIDE)
        block = rows_ref.at[tuple(index)]
        k = number[p, g, phase, kind]
        return pltpu.make_async_remote_copy(
            src_ref=block,
            dst_ref=block,
            send_sem=send_sem.at[k],
            recv_sem=take_sem.at[k],
            device_id=peer(axis, up),
            device_id_type=MESH,
        )

    def send(*key):
        copy = message(*key, False)
        copy.start()
        sent.append(copy)

    def multiply(p, g, kind):
        first, many = FIRST_TILE[p, g], GROUPS[p][g]
        if kind == 3:
            head_copies[p, g].wait()
        axis = ROUTES[p][2]
        plane = [slice(None)] * 3
        plane[axis] = lax.rem(at[axis] + (3, 1, 2, 0)[kind], SIDE)
        count = SIDE * SIDE * hidden_ref.shape[0]
        left = jnp.concatenate(
            [rows_ref[(first + k, *plane)].reshape(count, LANES) for k in range(many)], axis=1
        )
        product = jnp.dot(
            left, head_ref[first * LANES : (first + many) * LANES, :], preferred_element_type=jnp.float32
        )
        index = tuple(plane)
        logits_ref[index] += product.reshape(SIDE, SIDE, hidden_ref.shape[0], width)

    def put(ref, stage, axis, values):
        for k, value in enumerate(values):
            ref[stage, at[axis], k] = value

    def swap(ref, stage, number_of, axis):
        copies = []
        for step in (1, 2, 3):
            block = ref.at[stage, at[axis]]
            copy = pltpu.make_async_remote_copy(
                src_ref=block,
                dst_ref=block,
                send_sem=swap_send_sem.at[number_of, step - 1],
                recv_sem=swap_take_sem.at[number_of, step - 1],
                device_id=peer(axis, step),
                device_id_type=MESH,
            )
            copy.start()
            copies.append(copy)
        sent.extend(copies)
        return copies

    def taken(ref, stage, number_of, axis):
        for step in (1, 2, 3):
            block = ref.at[stage, lax.rem(at[axis] + SIDE - step, SIDE)]
            pltpu.make_async_remote_copy(
                src_ref=block,
                dst_ref=block,
                send_sem=swap_send_sem.at[number_of, step - 1],
                recv_sem=swap_take_sem.at[number_of, step - 1],
                device_id=peer(axis, step),
                device_id_type=MESH,
            ).wait_recv()

    def joined_pair(stage):
        tops = [pair_ref[stage, c, 0] for c in range(SIDE)]
        top = jnp.maximum(jnp.maximum(tops[0], tops[1]), jnp.maximum(tops[2], tops[3]))
        total = sum(pair_ref[stage, c, 1] * jnp.exp(tops[c] - top) for c in range(SIDE))
        return top, total, sum(pair_ref[stage, c, 2] for c in range(SIDE))

    shifts = sorted(
        (o for o in itertools.product(range(SIDE), repeat=3) if any(o)), key=lambda o: -sum(min(v, SIDE - v) for v in o)
    )

    def across(turn, k, back):
        there = me
        for axis in range(3):
            step = shifts[k][axis]
            here = lax.rem(at[axis] + (SIDE - step if back else step), SIDE)
            there = there + (here - at[axis]) * stride[axis]
        block = bank_ref.at[turn, there if back else me]
        return pltpu.make_async_remote_copy(
            src_ref=block,
            dst_ref=block,
            send_sem=far_send_sem.at[turn, k],
            recv_sem=far_take_sem.at[turn, k],
            device_id=(there, batch),
            device_id_type=MESH,
        )

    def cast(turn, value):
        bank_ref[turn, me] = value
        for k in range(len(shifts)):
            copy = across(turn, k, False)
            copy.start()
            sent.append(copy)

    def collected(turn):
        for k in range(len(shifts)):
            across(turn, k, True).wait_recv()
        return [bank_ref[turn, v] for v in range(len(shifts) + 1)]

    def joined_lse(values):
        top = values[0]
        for value in values[1:]:
            top = jnp.maximum(top, value)
        return top + jnp.log(sum(jnp.exp(value - top) for value in values))

    def rows_of(b):
        return pl.ds(pl.multiple_of(b * LANES, LANES), LANES)

    def logits_at(b, tile):
        block = logits_ref[b // 2, pl.ds(lax.rem(b, 2) * 2, 2), :, :, tile]
        return block.reshape(LANES, tile.stop - tile.start)

    def stat_row(k, b):
        return stat_ref[k, pl.ds(b, 1), :]

    def set_stat(k, b, value):
        stat_ref[k, pl.ds(b, 1), :] = value

    def down(matrix, combine):
        return combine(jnp.transpose(matrix), axis=0, keepdims=True)

    lane = lax.broadcasted_iota(jnp.int32, (LANES, LANES), 1).astype(jnp.float32)

    def pickers(b):
        parent = as_column(parents_ref[pl.ds(b, 1), :].astype(jnp.float32))
        below = (lax.broadcasted_iota(jnp.int32, (LANES, LANES), 0) // NODES * NODES).astype(jnp.float32)
        hot = jnp.where(parent + below == lane, 1.0, 0.0).astype(jnp.bfloat16)
        token = as_column((tokens_ref[pl.ds(b, 1), :] - me * width).astype(jnp.float32))
        return hot, token

    def picked(pieces, hot, token):
        total = jnp.zeros((LANES, LANES), jnp.float32)
        for c in range(width // 256):
            found = sum(
                jnp.dot(hot, piece, preferred_element_type=jnp.float32)
                for piece in pieces(slice(c * 256, (c + 1) * 256))
            )
            for half in range(2):
                here = found[:, half * LANES : (half + 1) * LANES]
                total += jnp.where(token == lane + float(c * 256 + half * LANES), here, 0.0)
        return total

    def column_tiles():
        return [slice(c * LANES, (c + 1) * LANES) for c in range(width // LANES)]

    def draft_stats(b, carry):
        rows = rows_of(b)
        top = jnp.full((LANES, LANES), -jnp.inf, jnp.float32)
        for tile in column_tiles():
            top = jnp.maximum(top, draft_ref[rows, tile].astype(jnp.float32))
        top = down(top, jnp.max)
        column = as_column(top)
        total = jnp.zeros((LANES, LANES), jnp.float32)
        for tile in column_tiles():
            total += jnp.exp(draft_ref[rows, tile].astype(jnp.float32) - column)
        set_stat(0, b, top)
        set_stat(1, b, down(total, jnp.sum))
        hot, token = pickers(b)
        set_stat(2, b, down(picked(lambda tile: [draft_ref[rows, tile]], hot, token), jnp.sum))
        return carry

    def draft_probs(b, carry):
        rows = rows_of(b)
        column = as_column(stat_row(6, b))
        for tile in column_tiles():
            draft_prob_ref[rows, tile] = jnp.exp(draft_ref[rows, tile].astype(jnp.float32) - column)
        return carry

    def target_stats(b, carry):
        rows = rows_of(b)
        top = jnp.full((LANES, LANES), -jnp.inf, jnp.float32)
        for tile in column_tiles():
            top = jnp.maximum(top, logits_at(b, tile))
        top = down(top, jnp.max)
        column = as_column(top)
        total = jnp.zeros((LANES, LANES), jnp.float32)
        for tile in column_tiles():
            weight = jnp.exp(logits_at(b, tile) - column)
            weight_ref[rows, tile] = weight
            total += weight
        set_stat(3, b, top)
        set_stat(4, b, down(total, jnp.sum))
        return carry

    def target_picks(b, carry):
        rows = rows_of(b)

        def pieces(tile):
            values = logits_at(b, tile)
            high = values.astype(jnp.bfloat16)
            rest = values - high.astype(jnp.float32)
            middle = rest.astype(jnp.bfloat16)
            low = (rest - middle.astype(jnp.float32)).astype(jnp.bfloat16)
            return high, middle, low

        hot, token = pickers(b)
        set_stat(5, b, down(picked(pieces, hot, token), jnp.sum))
        return carry

    def residuals(b, carry):
        rows = rows_of(b)
        factor = as_column(stat_row(7, b))
        total = jnp.zeros((LANES, LANES), jnp.float32)
        for tile in column_tiles():
            total += jnp.maximum(weight_ref[rows, tile] * factor - draft_prob_ref[rows, tile], 0.0)
        set_stat(8, b, down(total, jnp.sum))
        return carry

    def over(body, unroll):
        lax.fori_loop(0, spans, body, 0, unroll=unroll)

    def work_on_draft(what, which):
        if what == "stats":
            if which == 0:
                for copy in small[2:]:
                    copy.wait()
            draft_stats(which, 0)
        elif what == "probs":
            draft_probs(which, 0)
        else:
            if which:
                taken(pair_ref, which - 1, which - 1, which - 1)
            values = joined_pair(which - 1) if which else (stat_ref[0], stat_ref[1], stat_ref[2])
            if which < 3:
                put(pair_ref, which, which, values)
                swap(pair_ref, which, which, which)
            else:
                stat_ref[6] = values[0] + jnp.log(values[1])
                out_ref[1] = stat_ref[6]
                out_ref[4] = values[2]

    for g in range(max(map(len, GROUPS))):
        for p in range(3):
            if g < len(GROUPS[p]):
                send(p, g, 0, 0)
                send(p, g, 0, 1)
    have = set()
    for kind, key in ORDER:
        if kind == "multiply":
            multiply(*key)
        elif kind == "draft":
            work_on_draft(*key)
        else:
            message(*key, True).wait_recv()
            p, g, phase, way = key
            have.add(key)
            if way == SIDES[p, g, phase]:
                send(p, g, phase, 2)
            if phase < 2 and all((p, g, phase, k) in have for k in range(3)):
                send(p, g, phase + 1, 0)
                send(p, g, phase + 1, 1)

    over(target_stats, spans)
    cast(0, stat_ref[3] + jnp.log(stat_ref[4]))
    over(target_picks, 2)
    cast(1, stat_ref[5])
    target_lse = joined_lse(collected(0))
    stat_ref[7] = jnp.exp(stat_ref[3] - target_lse)
    over(residuals, spans)
    cast(2, stat_ref[8])
    out_ref[0] = target_lse
    out_ref[3] = sum(collected(1))
    out_ref[2] = sum(collected(2))
    for copy in sent:
        copy.wait_send()


def tree_kernel(stats_ref, parents_ref, depths_ref, uniforms_ref, lse_ref, token_ref, residual_ref, accept_ref, path_ref):
    lanes = lax.broadcasted_iota(jnp.int32, parents_ref.shape, 1)
    parent = lanes // NODES * NODES + parents_ref[...]

    def at_parent(vector):
        return jnp.take_along_axis(vector, parent, axis=1)

    target_lse = stats_ref[0]
    token_logprob = stats_ref[3] - at_parent(target_lse)
    draft_logprob = stats_ref[4] - at_parent(stats_ref[1])
    accept = jnp.exp(jnp.minimum(token_logprob - draft_logprob, 0.0)) - uniforms_ref[...]
    depths = depths_ref[...]
    path = jnp.ones(accept.shape, jnp.float32)
    for level in range(1, DEPTH_MAX + 1):
        path = jnp.where(depths == level, jnp.minimum(accept, at_parent(path)), path)
    lse_ref[...] = target_lse
    token_ref[...] = token_logprob
    residual_ref[...] = stats_ref[2]
    accept_ref[...] = accept
    path_ref[...] = path


def body(hidden, norm_gain, lm_head, draft_logits, draft_tokens, tree_parents, node_depths, uniforms):
    depth, width = lm_head.shape
    rows = draft_logits.shape[0]
    spans = rows // LANES
    flat = (spans, LANES)
    hbm = pl.BlockSpec(memory_space=pltpu.HBM)
    vmem = pl.BlockSpec(memory_space=pltpu.VMEM)
    stats = pl.pallas_call(
        main_kernel,
        out_shape=jax.ShapeDtypeStruct((5, *flat), jnp.float32),
        in_specs=[hbm] * 6,
        out_specs=vmem,
        scratch_shapes=[
            pltpu.VMEM(hidden.shape, jnp.bfloat16),
            pltpu.VMEM((depth // LANES, LANES), jnp.bfloat16),
            pltpu.VMEM((depth, width), jnp.bfloat16),
            pltpu.VMEM((rows, width), jnp.bfloat16),
            pltpu.VMEM(flat, jnp.int32),
            pltpu.VMEM(flat, jnp.int32),
            pltpu.VMEM((depth // LANES, SIDE, SIDE, SIDE, hidden.shape[0], LANES), jnp.bfloat16),
            pltpu.VMEM((SIDE, SIDE, SIDE, hidden.shape[0], width), jnp.float32),
            pltpu.VMEM((rows, width), jnp.float32),
            pltpu.VMEM((rows, width), jnp.float32),
            pltpu.VMEM((9, *flat), jnp.float32),
            pltpu.VMEM((3, SIDE, 3, *flat), jnp.float32),
            pltpu.VMEM((3, SIDE**3, *flat), jnp.float32),
            pltpu.SemaphoreType.DMA((5,)),
            pltpu.SemaphoreType.DMA((len(PAIRS),)),
            pltpu.SemaphoreType.DMA((len(MESSAGES),)),
            pltpu.SemaphoreType.DMA((len(MESSAGES),)),
            pltpu.SemaphoreType.DMA((3, 3)),
            pltpu.SemaphoreType.DMA((3, 3)),
            pltpu.SemaphoreType.DMA((3, SIDE**3 - 1)),
            pltpu.SemaphoreType.DMA((3, SIDE**3 - 1)),
        ],
        compiler_params=pltpu.CompilerParams(
            collective_id=0, has_side_effects=True, vmem_limit_bytes=60 * 2**20
        ),
        name="gather_verify",
    )(
        hidden,
        norm_gain.reshape(depth // LANES, LANES),
        lm_head,
        draft_logits,
        draft_tokens.reshape(flat),
        tree_parents.reshape(flat),
    )
    outs = pl.pallas_call(
        tree_kernel,
        out_shape=[jax.ShapeDtypeStruct(flat, jnp.float32)] * 5,
        in_specs=[vmem] * 4,
        out_specs=[vmem] * 5,
        name="tree",
    )(stats, tree_parents.reshape(flat), node_depths.reshape(flat), uniforms.reshape(flat))
    return tuple(out.reshape(rows) for out in outs)


def solution(mesh):
    return jax.shard_map(
        body,
        mesh=mesh,
        in_specs=(
            P(("batch", "vocab"), None),
            P(),
            P(None, "vocab"),
            P("batch", "vocab"),
            P("batch"),
            P("batch"),
            P("batch"),
            P("batch"),
        ),
        out_specs=(P("batch"), P("batch"), P("batch"), P("batch"), P("batch")),
        check_vma=False,
    )
```

```python
import heapq
import itertools

import jax
import jax.numpy as jnp
from jax import lax
from jax.experimental import pallas as pl
from jax.experimental.pallas import tpu as pltpu
from jax.sharding import PartitionSpec as P

NODES = 64
DEPTH_MAX = 8
EPSILON = 1e-06
LANES = 128
SIDE = 4
MESH = pl.DeviceIdType.MESH

ROUTES = ((0, 1, 2), (1, 2, 0), (2, 0, 1))
GROUPS = (
    ((3, 7, 9), (3, 7, 9), (3, 7, 6, 3)),
    ((3, 7, 9), (3, 7, 9), (3, 7, 6, 3)),
    ((3, 6, 9), (3, 6, 9), (3, 6, 6, 3)),
)


def offset(p, phase, g):
    return sum(sum(part[0]) for part in GROUPS[:p]) + sum(GROUPS[p][phase][:g])


def finer(p, phase, g):
    low = offset(p, phase, g)
    high = low + GROUPS[p][phase][g]
    return [k for k in range(len(GROUPS[p][phase + 1])) if low <= offset(p, phase + 1, k) < high]


def relay_sides():
    sides = {}
    for p, part in enumerate(GROUPS):
        for phase, sizes in enumerate(part):
            lean = 0
            for g in sorted(range(len(sizes)), key=lambda g: -sizes[g]):
                sides[p, g, phase] = 0 if lean <= 0 else 1
                lean += sizes[g] if lean <= 0 else -sizes[g]
    return sides


SIDES = relay_sides()


def kinds_sent(g, phase):
    return (2, 0, 1) if phase == 0 or g == 0 and phase < 2 else (0, 1)


def passed_on(message):
    p, g, phase, kind = message
    return kind == SIDES[p, g, phase] and 2 not in kinds_sent(g, phase)


DRAFT = (
    [(("stats", b), 0.45, 2.0 if b == 0 else 0.0) for b in range(8)]
    + [(("join", axis), 0.3, 12.0 if axis else 0.0) for axis in range(4)]
    + [(("probs", b), 0.2, 0.0) for b in range(8)]
)


def plan():
    rate, gap, latency = 44500.0, 0.15, 2.2
    free = {(a, d): 0.0 for a in range(3) for d in range(2)}
    coming, count, have, order, ready = [], itertools.count(), set(), [], []
    draft = list(DRAFT)

    def send(now, p, g, phase, kind):
        way = (ROUTES[p][phase], kind if kind < 2 else SIDES[p, g, phase])
        free[way] = max(now, free[way]) + gap + GROUPS[p][phase][g] * 4096 * SIDE**phase / rate
        heapq.heappush(coming, (free[way] + latency, next(count), (p, g, phase, kind)))

    now, last = 0.0, 0.0
    for g in range(len(GROUPS[0][0])):
        for p in range(3):
            for kind in kinds_sent(g, 0):
                send(now, p, g, 0, kind)
    while coming or ready or draft:
        due = last + draft[0][2] if draft else float("inf")
        if coming and coming[0][0] <= now or not ready and coming and coming[0][0] <= due:
            at, _, message = heapq.heappop(coming)
            now = max(now, at) + 0.05
            p, g, phase, kind = message
            have.add(message)
            order.append(("take", message))
            if passed_on(message):
                send(now, p, g, phase, 2)
            if all((p, g, phase, k) in have for k in range(3)):
                for k in finer(p, phase, g) if phase < 2 else ():
                    for way in kinds_sent(k, phase + 1):
                        send(now, p, k, phase + 1, way)
                    if phase == 1:
                        ready.append((p, k, 3))
            if phase == 2:
                ready.append((p, g, kind))
        elif draft and (due <= now or not ready):
            what, cost, _ = draft.pop(0)
            order.append(("draft", what))
            now = last = max(now, due) + cost
        else:
            p, g, kind = ready.pop(0)
            order.append(("multiply", (p, g, kind)))
            now += 0.2 + 0.08 * max(2, GROUPS[p][2][g])
    return order


ORDER = plan()
PAIRS = [key[:2] for kind, key in ORDER if kind == "multiply" and key[2] == 3]
MESSAGES = [m for kind, m in ORDER if kind == "take"]


def as_column(row):
    return jnp.transpose(jnp.broadcast_to(row, (LANES, LANES)))


def main_kernel(
    hidden_hbm, gain_hbm, head_hbm, draft_hbm, tokens_hbm, parents_hbm,
    out_ref,
    hidden_ref, gain_ref, head_ref, draft_ref, tokens_ref, parents_ref,
    rows_ref, logits_ref, weight_ref, draft_prob_ref, stat_ref, pair_ref, bank_ref,
    small_sem, head_sem, send_sem, take_sem, swap_send_sem, swap_take_sem, far_send_sem, far_take_sem,
):
    me = lax.axis_index("vocab")
    batch = lax.axis_index("batch")
    at = (me // 16, (me // 4) % 4, me % 4)
    stride = (16, 4, 1)
    width = weight_ref.shape[1]
    spans = weight_ref.shape[0] // LANES

    def peer(axis, step):
        return (me + (lax.rem(at[axis] + step, SIDE) - at[axis]) * stride[axis], batch)

    small = [
        pltpu.make_async_copy(src, dst, small_sem.at[k])
        for k, (src, dst) in enumerate(
            (
                (hidden_hbm, hidden_ref),
                (gain_hbm, gain_ref),
                (draft_hbm, draft_ref),
                (tokens_hbm, tokens_ref),
                (parents_hbm, parents_ref),
            )
        )
    ]
    for copy in small:
        copy.start()
    barrier = pltpu.get_barrier_semaphore()
    for axis in range(3):
        for step in (2, 1, 3):
            pl.semaphore_signal(barrier, inc=1, device_id=peer(axis, step), device_id_type=MESH)
    head_copies = {}
    for k, pair in enumerate(PAIRS):
        span = pl.ds(offset(pair[0], 2, pair[1]) * LANES, GROUPS[pair[0]][2][pair[1]] * LANES)
        head_copies[pair] = pltpu.make_async_copy(head_hbm.at[span], head_ref.at[span], head_sem.at[k])
        head_copies[pair].start()

    small[0].wait()
    small[1].wait()
    tiles = hidden_ref.shape[1] // LANES
    squares = jnp.zeros((16, LANES), jnp.float32)
    for k in range(tiles):
        part = hidden_ref[:, k * LANES : (k + 1) * LANES].astype(jnp.float32)
        squares += part * part
    scale = lax.rsqrt(jnp.sum(squares, axis=1, keepdims=True) / hidden_ref.shape[1] + EPSILON)
    for k in range(tiles):
        part = hidden_ref[:, k * LANES : (k + 1) * LANES].astype(jnp.float32)
        gain = gain_ref[k : k + 1, :].astype(jnp.float32)
        rows_ref[k, at[0], at[1], at[2]] = (part * scale * gain).astype(jnp.bfloat16)
    for y in range(SIDE):
        logits_ref[y] = jnp.zeros(logits_ref.shape[1:], jnp.float32)
    pl.semaphore_wait(barrier, 9)

    number = {m: k for k, m in enumerate(MESSAGES)}
    sent = []

    def message(p, g, phase, kind, taking):
        axis = ROUTES[p][phase]
        side = kind if kind < 2 else SIDES[p, g, phase]
        up = 1 if side == 0 else 3
        routed = kind == 2 and 2 in kinds_sent(g, phase)
        begun = (SIDE - up) * (2 if kind == 2 else 1) if taking else ((SIDE - up) if kind == 2 and not routed else 0)
        index = [pl.ds(offset(p, phase, g), GROUPS[p][phase][g]), *at]
        for done in range(phase):
            index[1 + ROUTES[p][done]] = pl.ds(0, SIDE)
        index[1 + axis] = lax.rem(at[axis] + begun, SIDE)
        block = rows_ref.at[tuple(index)]
        k = number[p, g, phase, kind]
        return pltpu.make_async_remote_copy(
            src_ref=block,
            dst_ref=block,
            send_sem=send_sem.at[k],
            recv_sem=take_sem.at[k],
            device_id=peer(axis, 2 if routed else up),
            device_id_type=MESH,
        )

    def send(*key):
        copy = message(*key, False)
        copy.start()
        sent.append(copy)

    def multiply(p, g, kind):
        first, many = offset(p, 2, g), GROUPS[p][2][g]
        if kind == 3:
            head_copies[p, g].wait()
        axis = ROUTES[p][2]
        plane = [slice(None)] * 3
        plane[axis] = lax.rem(at[axis] + (3, 1, 2, 0)[kind], SIDE)
        count = SIDE * SIDE * hidden_ref.shape[0]
        left = jnp.concatenate(
            [rows_ref[(first + k, *plane)].reshape(count, LANES) for k in range(many)], axis=1
        )
        product = jnp.dot(
            left, head_ref[first * LANES : (first + many) * LANES, :], preferred_element_type=jnp.float32
        )
        index = tuple(plane)
        logits_ref[index] += product.reshape(SIDE, SIDE, hidden_ref.shape[0], width)

    def put(ref, stage, axis, values):
        for k, value in enumerate(values):
            ref[stage, at[axis], k] = value

    def swap(ref, stage, number_of, axis):
        copies = []
        for step in (1, 2, 3):
            block = ref.at[stage, at[axis]]
            copy = pltpu.make_async_remote_copy(
                src_ref=block,
                dst_ref=block,
                send_sem=swap_send_sem.at[number_of, step - 1],
                recv_sem=swap_take_sem.at[number_of, step - 1],
                device_id=peer(axis, step),
                device_id_type=MESH,
            )
            copy.start()
            copies.append(copy)
        sent.extend(copies)
        return copies

    def taken(ref, stage, number_of, axis):
        for step in (1, 2, 3):
            block = ref.at[stage, lax.rem(at[axis] + SIDE - step, SIDE)]
            pltpu.make_async_remote_copy(
                src_ref=block,
                dst_ref=block,
                send_sem=swap_send_sem.at[number_of, step - 1],
                recv_sem=swap_take_sem.at[number_of, step - 1],
                device_id=peer(axis, step),
                device_id_type=MESH,
            ).wait_recv()

    def joined_pair(stage):
        tops = [pair_ref[stage, c, 0] for c in range(SIDE)]
        top = jnp.maximum(jnp.maximum(tops[0], tops[1]), jnp.maximum(tops[2], tops[3]))
        total = sum(pair_ref[stage, c, 1] * jnp.exp(tops[c] - top) for c in range(SIDE))
        return top, total, sum(pair_ref[stage, c, 2] for c in range(SIDE))

    shifts = sorted(
        (o for o in itertools.product(range(SIDE), repeat=3) if any(o)), key=lambda o: -sum(min(v, SIDE - v) for v in o)
    )

    places = [[lax.rem(at[axis] + step, SIDE) * stride[axis] for step in range(SIDE)] for axis in range(3)]

    def across(turn, k, back):
        steps = [(SIDE - step) % SIDE if back else step for step in shifts[k]]
        there = sum(places[axis][step] for axis, step in enumerate(steps))
        block = bank_ref.at[turn, there if back else me]
        return pltpu.make_async_remote_copy(
            src_ref=block,
            dst_ref=block,
            send_sem=far_send_sem.at[turn, k],
            recv_sem=far_take_sem.at[turn, k],
            device_id=(there, batch),
            device_id_type=MESH,
        )

    def cast(turn, value):
        bank_ref[turn, me] = value
        for k in range(len(shifts)):
            copy = across(turn, k, False)
            copy.start()
            sent.append(copy)

    def collected(turn):
        for k in range(len(shifts)):
            across(turn, k, True).wait_recv()
        return [bank_ref[turn, v] for v in range(len(shifts) + 1)]

    def joined_lse(values):
        top = values[0]
        for value in values[1:]:
            top = jnp.maximum(top, value)
        return top + jnp.log(sum(jnp.exp(value - top) for value in values))

    def rows_of(b):
        return pl.ds(pl.multiple_of(b * LANES, LANES), LANES)

    def logits_at(b, tile):
        block = logits_ref[b // 2, pl.ds(lax.rem(b, 2) * 2, 2), :, :, tile]
        return block.reshape(LANES, tile.stop - tile.start)

    def stat_row(k, b):
        return stat_ref[k, pl.ds(b, 1), :]

    def set_stat(k, b, value):
        stat_ref[k, pl.ds(b, 1), :] = value

    def down(matrix, combine):
        return combine(jnp.transpose(matrix), axis=0, keepdims=True)

    lane = lax.broadcasted_iota(jnp.int32, (LANES, LANES), 1).astype(jnp.float32)

    def pickers(b):
        parent = as_column(parents_ref[pl.ds(b, 1), :].astype(jnp.float32))
        below = (lax.broadcasted_iota(jnp.int32, (LANES, LANES), 0) // NODES * NODES).astype(jnp.float32)
        hot = jnp.where(parent + below == lane, 1.0, 0.0).astype(jnp.bfloat16)
        token = as_column((tokens_ref[pl.ds(b, 1), :] - me * width).astype(jnp.float32))
        return hot, token

    def picked(pieces, hot, token):
        total = jnp.zeros((LANES, LANES), jnp.float32)
        for c in range(width // 256):
            found = sum(
                jnp.dot(hot, piece, preferred_element_type=jnp.float32)
                for piece in pieces(slice(c * 256, (c + 1) * 256))
            )
            for half in range(2):
                here = found[:, half * LANES : (half + 1) * LANES]
                total += jnp.where(token == lane + float(c * 256 + half * LANES), here, 0.0)
        return total

    def column_tiles():
        return [slice(c * LANES, (c + 1) * LANES) for c in range(width // LANES)]

    def draft_stats(b, carry):
        rows = rows_of(b)
        top = jnp.full((LANES, LANES), -jnp.inf, jnp.float32)
        for tile in column_tiles():
            top = jnp.maximum(top, draft_ref[rows, tile].astype(jnp.float32))
        top = down(top, jnp.max)
        column = as_column(top)
        total = jnp.zeros((LANES, LANES), jnp.float32)
        for tile in column_tiles():
            total += jnp.exp(draft_ref[rows, tile].astype(jnp.float32) - column)
        set_stat(0, b, top)
        set_stat(1, b, down(total, jnp.sum))
        hot, token = pickers(b)
        set_stat(2, b, down(picked(lambda tile: [draft_ref[rows, tile]], hot, token), jnp.sum))
        return carry

    def draft_probs(b, carry):
        rows = rows_of(b)
        column = as_column(stat_row(6, b))
        for tile in column_tiles():
            draft_prob_ref[rows, tile] = jnp.exp(draft_ref[rows, tile].astype(jnp.float32) - column)
        return carry

    def target_stats(b, carry):
        rows = rows_of(b)
        top = jnp.full((LANES, LANES), -jnp.inf, jnp.float32)
        for tile in column_tiles():
            top = jnp.maximum(top, logits_at(b, tile))
        top = down(top, jnp.max)
        column = as_column(top)
        total = jnp.zeros((LANES, LANES), jnp.float32)
        for tile in column_tiles():
            weight = jnp.exp(logits_at(b, tile) - column)
            weight_ref[rows, tile] = weight
            total += weight
        set_stat(3, b, top)
        set_stat(4, b, down(total, jnp.sum))
        return carry

    def target_picks(b, carry):
        rows = rows_of(b)

        def pieces(tile):
            values = logits_at(b, tile)
            high = values.astype(jnp.bfloat16)
            rest = values - high.astype(jnp.float32)
            middle = rest.astype(jnp.bfloat16)
            low = (rest - middle.astype(jnp.float32)).astype(jnp.bfloat16)
            return high, middle, low

        hot, token = pickers(b)
        set_stat(5, b, down(picked(pieces, hot, token), jnp.sum))
        return carry

    def residuals(b, carry):
        rows = rows_of(b)
        factor = as_column(stat_row(7, b))
        total = jnp.zeros((LANES, LANES), jnp.float32)
        for tile in column_tiles():
            total += jnp.maximum(weight_ref[rows, tile] * factor - draft_prob_ref[rows, tile], 0.0)
        set_stat(8, b, down(total, jnp.sum))
        return carry

    def over(body, unroll):
        lax.fori_loop(0, spans, body, 0, unroll=unroll)

    def work_on_draft(what, which):
        if what == "stats":
            if which == 0:
                for copy in small[2:]:
                    copy.wait()
            draft_stats(which, 0)
        elif what == "probs":
            draft_probs(which, 0)
        else:
            if which:
                taken(pair_ref, which - 1, which - 1, which - 1)
            values = joined_pair(which - 1) if which else (stat_ref[0], stat_ref[1], stat_ref[2])
            if which < 3:
                put(pair_ref, which, which, values)
                swap(pair_ref, which, which, which)
            else:
                stat_ref[6] = values[0] + jnp.log(values[1])
                out_ref[1] = stat_ref[6]
                out_ref[4] = values[2]

    for g in range(len(GROUPS[0][0])):
        for p in range(3):
            for kind in kinds_sent(g, 0):
                send(p, g, 0, kind)
    have = set()
    for kind, key in ORDER:
        if kind == "multiply":
            multiply(*key)
        elif kind == "draft":
            work_on_draft(*key)
        else:
            message(*key, True).wait_recv()
            p, g, phase, way = key
            have.add(key)
            if passed_on(key):
                send(p, g, phase, 2)
            if phase < 2 and all((p, g, phase, k) in have for k in range(3)):
                for k in finer(p, phase, g):
                    for to in kinds_sent(k, phase + 1):
                        send(p, k, phase + 1, to)

    over(target_stats, spans)
    cast(0, stat_ref[3] + jnp.log(stat_ref[4]))
    over(target_picks, 2)
    cast(1, stat_ref[5])
    far = 2 * len(shifts)
    for copy in sent[:-far]:
        copy.wait_send()
    del sent[:-far]
    target_lse = joined_lse(collected(0))
    stat_ref[7] = jnp.exp(stat_ref[3] - target_lse)
    over(residuals, spans)
    cast(2, stat_ref[8])
    for copy in sent[:far]:
        copy.wait_send()
    del sent[:far]
    out_ref[0] = target_lse
    out_ref[3] = sum(collected(1))
    out_ref[2] = sum(collected(2))
    for copy in sent:
        copy.wait_send()


def tree_kernel(stats_ref, parents_ref, depths_ref, uniforms_ref, lse_ref, token_ref, residual_ref, accept_ref, path_ref):
    lanes = lax.broadcasted_iota(jnp.int32, parents_ref.shape, 1)
    parent = lanes // NODES * NODES + parents_ref[...]

    def at_parent(vector):
        return jnp.take_along_axis(vector, parent, axis=1)

    target_lse = stats_ref[0]
    token_logprob = stats_ref[3] - at_parent(target_lse)
    draft_logprob = stats_ref[4] - at_parent(stats_ref[1])
    accept = jnp.exp(jnp.minimum(token_logprob - draft_logprob, 0.0)) - uniforms_ref[...]
    depths = depths_ref[...]
    path = jnp.ones(accept.shape, jnp.float32)
    for level in range(1, DEPTH_MAX + 1):
        path = jnp.where(depths == level, jnp.minimum(accept, at_parent(path)), path)
    lse_ref[...] = target_lse
    token_ref[...] = token_logprob
    residual_ref[...] = stats_ref[2]
    accept_ref[...] = accept
    path_ref[...] = path


def body(hidden, norm_gain, lm_head, draft_logits, draft_tokens, tree_parents, node_depths, uniforms):
    depth, width = lm_head.shape
    rows = draft_logits.shape[0]
    spans = rows // LANES
    flat = (spans, LANES)
    hbm = pl.BlockSpec(memory_space=pltpu.HBM)
    vmem = pl.BlockSpec(memory_space=pltpu.VMEM)
    stats = pl.pallas_call(
        main_kernel,
        out_shape=jax.ShapeDtypeStruct((5, *flat), jnp.float32),
        in_specs=[hbm] * 6,
        out_specs=vmem,
        scratch_shapes=[
            pltpu.VMEM(hidden.shape, jnp.bfloat16),
            pltpu.VMEM((depth // LANES, LANES), jnp.bfloat16),
            pltpu.VMEM((depth, width), jnp.bfloat16),
            pltpu.VMEM((rows, width), jnp.bfloat16),
            pltpu.VMEM(flat, jnp.int32),
            pltpu.VMEM(flat, jnp.int32),
            pltpu.VMEM((depth // LANES, SIDE, SIDE, SIDE, hidden.shape[0], LANES), jnp.bfloat16),
            pltpu.VMEM((SIDE, SIDE, SIDE, hidden.shape[0], width), jnp.float32),
            pltpu.VMEM((rows, width), jnp.float32),
            pltpu.VMEM((rows, width), jnp.float32),
            pltpu.VMEM((9, *flat), jnp.float32),
            pltpu.VMEM((3, SIDE, 3, *flat), jnp.float32),
            pltpu.VMEM((3, SIDE**3, *flat), jnp.float32),
            pltpu.SemaphoreType.DMA((5,)),
            pltpu.SemaphoreType.DMA((len(PAIRS),)),
            pltpu.SemaphoreType.DMA((len(MESSAGES),)),
            pltpu.SemaphoreType.DMA((len(MESSAGES),)),
            pltpu.SemaphoreType.DMA((3, 3)),
            pltpu.SemaphoreType.DMA((3, 3)),
            pltpu.SemaphoreType.DMA((3, SIDE**3 - 1)),
            pltpu.SemaphoreType.DMA((3, SIDE**3 - 1)),
        ],
        compiler_params=pltpu.CompilerParams(
            collective_id=0, has_side_effects=True, vmem_limit_bytes=60 * 2**20
        ),
        name="gather_verify",
    )(
        hidden,
        norm_gain.reshape(depth // LANES, LANES),
        lm_head,
        draft_logits,
        draft_tokens.reshape(flat),
        tree_parents.reshape(flat),
    )
    outs = pl.pallas_call(
        tree_kernel,
        out_shape=[jax.ShapeDtypeStruct(flat, jnp.float32)] * 5,
        in_specs=[vmem] * 4,
        out_specs=[vmem] * 5,
        name="tree",
    )(stats, tree_parents.reshape(flat), node_depths.reshape(flat), uniforms.reshape(flat))
    return tuple(out.reshape(rows) for out in outs)


def solution(mesh):
    return jax.shard_map(
        body,
        mesh=mesh,
        in_specs=(
            P(("batch", "vocab"), None),
            P(),
            P(None, "vocab"),
            P("batch", "vocab"),
            P("batch"),
            P("batch"),
            P("batch"),
            P("batch"),
        ),
        out_specs=(P("batch"), P("batch"), P("batch"), P("batch"), P("batch")),
        check_vma=False,
    )
```

```python
import heapq
import itertools

import jax
import jax.numpy as jnp
from jax import lax
from jax.experimental import pallas as pl
from jax.experimental.pallas import tpu as pltpu
from jax.sharding import PartitionSpec as P

NODES = 64
DEPTH_MAX = 8
EPSILON = 1e-06
LANES = 128
SIDE = 4
MESH = pl.DeviceIdType.MESH

ROUTES = ((0, 1, 2), (1, 2, 0), (2, 0, 1))
GROUPS = (
    ((3, 6, 10), (3, 6, 10), (3, 6, 5, 3, 2)),
    ((3, 6, 10), (3, 6, 10), (3, 6, 5, 3, 2)),
    ((3, 6, 9), (3, 6, 9), (3, 6, 4, 3, 2)),
)


def offset(p, phase, g):
    return sum(sum(part[0]) for part in GROUPS[:p]) + sum(GROUPS[p][phase][:g])


def finer(p, phase, g):
    low = offset(p, phase, g)
    high = low + GROUPS[p][phase][g]
    return [k for k in range(len(GROUPS[p][phase + 1])) if low <= offset(p, phase + 1, k) < high]


def relay_sides():
    sides = {}
    for p, part in enumerate(GROUPS):
        for phase, sizes in enumerate(part):
            lean = 0
            for g in sorted(range(len(sizes)), key=lambda g: -sizes[g]):
                sides[p, g, phase] = 0 if lean <= 0 else 1
                lean += sizes[g] if lean <= 0 else -sizes[g]
    return sides


SIDES = relay_sides()


def kinds_sent(g, phase):
    return (2, 0, 1) if phase == 0 or g == 0 and phase < 2 else (0, 1)


def passed_on(message):
    p, g, phase, kind = message
    return kind == SIDES[p, g, phase] and 2 not in kinds_sent(g, phase)


DRAFT = (
    [(("stats", b), 0.45, 2.0 if b == 0 else 0.0) for b in range(8)]
    + [(("join", axis), 0.3, 12.0 if axis else 0.0) for axis in range(4)]
    + [(("probs", b), 0.2, 0.0) for b in range(8)]
)


def plan():
    rate, gap, latency = 44500.0, 0.15, 2.2
    free = {(a, d): 0.0 for a in range(3) for d in range(2)}
    coming, count, have, order, ready = [], itertools.count(), set(), [], []
    draft = list(DRAFT)

    def send(now, p, g, phase, kind):
        way = (ROUTES[p][phase], kind if kind < 2 else SIDES[p, g, phase])
        free[way] = max(now, free[way]) + gap + GROUPS[p][phase][g] * 4096 * SIDE**phase / rate
        heapq.heappush(coming, (free[way] + latency, next(count), (p, g, phase, kind)))

    now, last = 0.0, 0.0
    for g in range(len(GROUPS[0][0])):
        for p in range(3):
            for kind in kinds_sent(g, 0):
                send(now, p, g, 0, kind)
    while coming or ready or draft:
        due = last + draft[0][2] if draft else float("inf")
        if coming and coming[0][0] <= now or not ready and coming and coming[0][0] <= due:
            at, _, message = heapq.heappop(coming)
            now = max(now, at) + 0.05
            p, g, phase, kind = message
            have.add(message)
            order.append(("take", message))
            if passed_on(message):
                send(now, p, g, phase, 2)
            if all((p, g, phase, k) in have for k in range(3)):
                for k in finer(p, phase, g) if phase < 2 else ():
                    for way in kinds_sent(k, phase + 1):
                        send(now, p, k, phase + 1, way)
                    if phase == 1:
                        ready.append((p, k, 3))
            if phase == 2:
                ready.append((p, g, kind))
        elif draft and (due <= now or not ready):
            what, cost, _ = draft.pop(0)
            order.append(("draft", what))
            now = last = max(now, due) + cost
        else:
            p, g, kind = ready.pop(0)
            order.append(("multiply", (p, g, kind)))
            now += 0.2 + 0.08 * max(2, GROUPS[p][2][g])
    return order


ORDER = plan()
PAIRS = [key[:2] for kind, key in ORDER if kind == "multiply" and key[2] == 3]
MESSAGES = [m for kind, m in ORDER if kind == "take"]


def as_column(row):
    return jnp.transpose(jnp.broadcast_to(row, (LANES, LANES)))


def main_kernel(
    hidden_hbm, gain_hbm, head_hbm, draft_hbm, tokens_hbm, parents_hbm,
    out_ref,
    hidden_ref, gain_ref, head_ref, draft_ref, tokens_ref, parents_ref,
    rows_ref, logits_ref, weight_ref, draft_prob_ref, stat_ref, pair_ref, pick_ref, bank_ref,
    small_sem, head_sem, send_sem, take_sem, swap_send_sem, swap_take_sem, far_send_sem, far_take_sem,
):
    me = lax.axis_index("vocab")
    batch = lax.axis_index("batch")
    at = (me // 16, (me // 4) % 4, me % 4)
    stride = (16, 4, 1)
    width = weight_ref.shape[1]
    spans = weight_ref.shape[0] // LANES

    def peer(axis, step):
        return (me + (lax.rem(at[axis] + step, SIDE) - at[axis]) * stride[axis], batch)

    small = [
        pltpu.make_async_copy(src, dst, small_sem.at[k])
        for k, (src, dst) in enumerate(
            (
                (hidden_hbm, hidden_ref),
                (gain_hbm, gain_ref),
                (draft_hbm, draft_ref),
                (tokens_hbm, tokens_ref),
                (parents_hbm, parents_ref),
            )
        )
    ]
    for copy in small:
        copy.start()
    barrier = pltpu.get_barrier_semaphore()
    for axis in range(3):
        for step in (2, 1, 3):
            pl.semaphore_signal(barrier, inc=1, device_id=peer(axis, step), device_id_type=MESH)
    head_copies = {}
    for k, pair in enumerate(PAIRS):
        span = pl.ds(offset(pair[0], 2, pair[1]) * LANES, GROUPS[pair[0]][2][pair[1]] * LANES)
        head_copies[pair] = pltpu.make_async_copy(head_hbm.at[span], head_ref.at[span], head_sem.at[k])
        head_copies[pair].start()

    small[0].wait()
    small[1].wait()
    tiles = hidden_ref.shape[1] // LANES
    squares = jnp.zeros((16, LANES), jnp.float32)
    for k in range(tiles):
        part = hidden_ref[:, k * LANES : (k + 1) * LANES].astype(jnp.float32)
        squares += part * part
    scale = lax.rsqrt(jnp.sum(squares, axis=1, keepdims=True) / hidden_ref.shape[1] + EPSILON)
    for k in range(tiles):
        part = hidden_ref[:, k * LANES : (k + 1) * LANES].astype(jnp.float32)
        gain = gain_ref[k : k + 1, :].astype(jnp.float32)
        rows_ref[k, at[0], at[1], at[2]] = (part * scale * gain).astype(jnp.bfloat16)
    for y in range(SIDE):
        logits_ref[y] = jnp.zeros(logits_ref.shape[1:], jnp.float32)
    pl.semaphore_wait(barrier, 9)

    number = {m: k for k, m in enumerate(MESSAGES)}
    sent = []

    def message(p, g, phase, kind, taking):
        axis = ROUTES[p][phase]
        side = kind if kind < 2 else SIDES[p, g, phase]
        up = 1 if side == 0 else 3
        routed = kind == 2 and 2 in kinds_sent(g, phase)
        begun = (SIDE - up) * (2 if kind == 2 else 1) if taking else ((SIDE - up) if kind == 2 and not routed else 0)
        index = [pl.ds(offset(p, phase, g), GROUPS[p][phase][g]), *at]
        for done in range(phase):
            index[1 + ROUTES[p][done]] = pl.ds(0, SIDE)
        index[1 + axis] = lax.rem(at[axis] + begun, SIDE)
        block = rows_ref.at[tuple(index)]
        k = number[p, g, phase, kind]
        return pltpu.make_async_remote_copy(
            src_ref=block,
            dst_ref=block,
            send_sem=send_sem.at[k],
            recv_sem=take_sem.at[k],
            device_id=peer(axis, 2 if routed else up),
            device_id_type=MESH,
        )

    def send(*key):
        copy = message(*key, False)
        copy.start()
        sent.append(copy)

    def multiply(p, g, kind):
        first, many = offset(p, 2, g), GROUPS[p][2][g]
        if kind == 3:
            head_copies[p, g].wait()
        axis = ROUTES[p][2]
        plane = [slice(None)] * 3
        plane[axis] = lax.rem(at[axis] + (3, 1, 2, 0)[kind], SIDE)
        count = SIDE * SIDE * hidden_ref.shape[0]
        left = jnp.concatenate(
            [rows_ref[(first + k, *plane)].reshape(count, LANES) for k in range(many)], axis=1
        )
        product = jnp.dot(
            left, head_ref[first * LANES : (first + many) * LANES, :], preferred_element_type=jnp.float32
        )
        index = tuple(plane)
        logits_ref[index] += product.reshape(SIDE, SIDE, hidden_ref.shape[0], width)

    def put(ref, stage, axis, values):
        for k, value in enumerate(values):
            ref[stage, at[axis], k] = value

    def swap(ref, stage, number_of, axis):
        copies = []
        for step in (1, 2, 3):
            block = ref.at[stage, at[axis]]
            copy = pltpu.make_async_remote_copy(
                src_ref=block,
                dst_ref=block,
                send_sem=swap_send_sem.at[number_of, step - 1],
                recv_sem=swap_take_sem.at[number_of, step - 1],
                device_id=peer(axis, step),
                device_id_type=MESH,
            )
            copy.start()
            copies.append(copy)
        sent.extend(copies)
        return copies

    def taken(ref, stage, number_of, axis):
        for step in (1, 2, 3):
            block = ref.at[stage, lax.rem(at[axis] + SIDE - step, SIDE)]
            pltpu.make_async_remote_copy(
                src_ref=block,
                dst_ref=block,
                send_sem=swap_send_sem.at[number_of, step - 1],
                recv_sem=swap_take_sem.at[number_of, step - 1],
                device_id=peer(axis, step),
                device_id_type=MESH,
            ).wait_recv()

    def joined_pair(stage):
        tops = [pair_ref[stage, c, 0] for c in range(SIDE)]
        top = jnp.maximum(jnp.maximum(tops[0], tops[1]), jnp.maximum(tops[2], tops[3]))
        total = sum(pair_ref[stage, c, 1] * jnp.exp(tops[c] - top) for c in range(SIDE))
        return top, total, sum(pair_ref[stage, c, 2] for c in range(SIDE))

    shifts = sorted(
        (o for o in itertools.product(range(SIDE), repeat=3) if any(o)), key=lambda o: -sum(min(v, SIDE - v) for v in o)
    )

    places = [[lax.rem(at[axis] + step, SIDE) * stride[axis] for step in range(SIDE)] for axis in range(3)]

    def across(turn, k, back):
        steps = [(SIDE - step) % SIDE if back else step for step in shifts[k]]
        there = sum(places[axis][step] for axis, step in enumerate(steps))
        block = bank_ref.at[turn, there if back else me]
        return pltpu.make_async_remote_copy(
            src_ref=block,
            dst_ref=block,
            send_sem=far_send_sem.at[turn, k],
            recv_sem=far_take_sem.at[turn, k],
            device_id=(there, batch),
            device_id_type=MESH,
        )

    def cast(turn, value):
        bank_ref[turn, me] = value
        for k in range(len(shifts)):
            copy = across(turn, k, False)
            copy.start()
            sent.append(copy)

    def collected(turn):
        for k in range(len(shifts)):
            across(turn, k, True).wait_recv()
        return [bank_ref[turn, v] for v in range(len(shifts) + 1)]

    def joined_lse(values):
        top = values[0]
        for value in values[1:]:
            top = jnp.maximum(top, value)
        return top + jnp.log(sum(jnp.exp(value - top) for value in values))

    def rows_of(b):
        return pl.ds(pl.multiple_of(b * LANES, LANES), LANES)

    def logits_at(b, tile):
        block = logits_ref[b // 2, pl.ds(lax.rem(b, 2) * 2, 2), :, :, tile]
        return block.reshape(LANES, tile.stop - tile.start)

    def stat_row(k, b):
        return stat_ref[k, pl.ds(b, 1), :]

    def set_stat(k, b, value):
        stat_ref[k, pl.ds(b, 1), :] = value

    def down(matrix, combine):
        return combine(jnp.transpose(matrix), axis=0, keepdims=True)

    lane = lax.broadcasted_iota(jnp.int32, (LANES, LANES), 1).astype(jnp.float32)

    def pickers(b):
        parent = as_column(parents_ref[pl.ds(b, 1), :].astype(jnp.float32))
        below = (lax.broadcasted_iota(jnp.int32, (LANES, LANES), 0) // NODES * NODES).astype(jnp.float32)
        hot = jnp.where(parent + below == lane, 1.0, 0.0).astype(jnp.bfloat16)
        token = as_column((tokens_ref[pl.ds(b, 1), :] - me * width).astype(jnp.float32))
        return hot, token

    def picked(pieces, hot, token):
        total = jnp.zeros((LANES, LANES), jnp.float32)
        for c in range(width // 256):
            found = sum(
                jnp.dot(hot, piece, preferred_element_type=jnp.float32)
                for piece in pieces(slice(c * 256, (c + 1) * 256))
            )
            for half in range(2):
                here = found[:, half * LANES : (half + 1) * LANES]
                total += jnp.where(token == lane + float(c * 256 + half * LANES), here, 0.0)
        return total

    def column_tiles():
        return [slice(c * LANES, (c + 1) * LANES) for c in range(width // LANES)]

    def draft_stats(b, carry):
        rows = rows_of(b)
        top = jnp.full((LANES, LANES), -jnp.inf, jnp.float32)
        for tile in column_tiles():
            top = jnp.maximum(top, draft_ref[rows, tile].astype(jnp.float32))
        top = down(top, jnp.max)
        column = as_column(top)
        total = jnp.zeros((LANES, LANES), jnp.float32)
        for tile in column_tiles():
            total += jnp.exp(draft_ref[rows, tile].astype(jnp.float32) - column)
        set_stat(0, b, top)
        set_stat(1, b, down(total, jnp.sum))
        hot, token = pickers(b)
        set_stat(2, b, down(picked(lambda tile: [draft_ref[rows, tile]], hot, token), jnp.sum))
        return carry

    def draft_probs(b, carry):
        rows = rows_of(b)
        column = as_column(stat_row(6, b))
        for tile in column_tiles():
            draft_prob_ref[rows, tile] = jnp.exp(draft_ref[rows, tile].astype(jnp.float32) - column)
        return carry

    def target_stats(b, carry):
        rows = rows_of(b)
        top = jnp.full((LANES, LANES), -jnp.inf, jnp.float32)
        for tile in column_tiles():
            top = jnp.maximum(top, logits_at(b, tile))
        top = down(top, jnp.max)
        column = as_column(top)
        total = jnp.zeros((LANES, LANES), jnp.float32)
        for tile in column_tiles():
            weight = jnp.exp(logits_at(b, tile) - column)
            weight_ref[rows, tile] = weight
            total += weight
        set_stat(3, b, top)
        set_stat(4, b, down(total, jnp.sum))
        return carry

    def target_picks(b, carry):
        rows = rows_of(b)

        def pieces(tile):
            values = logits_at(b, tile)
            high = values.astype(jnp.bfloat16)
            rest = values - high.astype(jnp.float32)
            middle = rest.astype(jnp.bfloat16)
            low = (rest - middle.astype(jnp.float32)).astype(jnp.bfloat16)
            return high, middle, low

        hot, token = pickers(b)
        set_stat(5, b, down(picked(pieces, hot, token), jnp.sum))
        return carry

    def residuals(b, carry):
        rows = rows_of(b)
        factor = as_column(stat_row(7, b))
        total = jnp.zeros((LANES, LANES), jnp.float32)
        for tile in column_tiles():
            total += jnp.maximum(weight_ref[rows, tile] * factor - draft_prob_ref[rows, tile], 0.0)
        set_stat(8, b, down(total, jnp.sum))
        return carry

    def over(body, unroll):
        lax.fori_loop(0, spans, body, 0, unroll=unroll)

    def work_on_draft(what, which):
        if what == "stats":
            if which == 0:
                for copy in small[2:]:
                    copy.wait()
            draft_stats(which, 0)
        elif what == "probs":
            draft_probs(which, 0)
        else:
            if which:
                taken(pair_ref, which - 1, which - 1, which - 1)
            values = joined_pair(which - 1) if which else (stat_ref[0], stat_ref[1], stat_ref[2])
            if which < 3:
                put(pair_ref, which, which, values)
                swap(pair_ref, which, which, which)
            else:
                stat_ref[6] = values[0] + jnp.log(values[1])
                out_ref[1] = stat_ref[6]
                out_ref[4] = values[2]

    for g in range(len(GROUPS[0][0])):
        for p in range(3):
            for kind in kinds_sent(g, 0):
                send(p, g, 0, kind)
    have = set()
    for kind, key in ORDER:
        if kind == "multiply":
            multiply(*key)
        elif kind == "draft":
            work_on_draft(*key)
        else:
            message(*key, True).wait_recv()
            p, g, phase, way = key
            have.add(key)
            if passed_on(key):
                send(p, g, phase, 2)
            if phase < 2 and all((p, g, phase, k) in have for k in range(3)):
                for k in finer(p, phase, g):
                    for to in kinds_sent(k, phase + 1):
                        send(p, k, phase + 1, to)

    over(target_stats, spans)
    cast(0, stat_ref[3] + jnp.log(stat_ref[4]))
    over(target_picks, 2)
    def pick_sum(stage):
        taken(pick_ref, stage, 3 + stage, stage)
        return sum(pick_ref[stage, c, 0] for c in range(SIDE))

    put(pick_ref, 0, 0, (stat_ref[5],))
    swap(pick_ref, 0, 3, 0)
    early = len(sent) - len(shifts) - 3
    for copy in sent[:early]:
        copy.wait_send()
    del sent[:early]
    put(pick_ref, 1, 1, (pick_sum(0),))
    swap(pick_ref, 1, 4, 1)
    target_lse = joined_lse(collected(0))
    stat_ref[7] = jnp.exp(stat_ref[3] - target_lse)
    over(residuals, spans)
    cast(1, stat_ref[8])
    out_ref[0] = target_lse
    early = len(sent) - len(shifts)
    for copy in sent[:early]:
        copy.wait_send()
    del sent[:early]
    put(pick_ref, 2, 2, (pick_sum(1),))
    swap(pick_ref, 2, 5, 2)
    out_ref[3] = pick_sum(2)
    out_ref[2] = sum(collected(1))
    for copy in sent:
        copy.wait_send()


def tree_kernel(stats_ref, parents_ref, depths_ref, uniforms_ref, lse_ref, token_ref, residual_ref, accept_ref, path_ref):
    lanes = lax.broadcasted_iota(jnp.int32, parents_ref.shape, 1)
    parent = lanes // NODES * NODES + parents_ref[...]

    def at_parent(vector):
        return jnp.take_along_axis(vector, parent, axis=1)

    target_lse = stats_ref[0]
    token_logprob = stats_ref[3] - at_parent(target_lse)
    draft_logprob = stats_ref[4] - at_parent(stats_ref[1])
    accept = jnp.exp(jnp.minimum(token_logprob - draft_logprob, 0.0)) - uniforms_ref[...]
    depths = depths_ref[...]
    path = jnp.ones(accept.shape, jnp.float32)
    for level in range(1, DEPTH_MAX + 1):
        path = jnp.where(depths == level, jnp.minimum(accept, at_parent(path)), path)
    lse_ref[...] = target_lse
    token_ref[...] = token_logprob
    residual_ref[...] = stats_ref[2]
    accept_ref[...] = accept
    path_ref[...] = path


def body(hidden, norm_gain, lm_head, draft_logits, draft_tokens, tree_parents, node_depths, uniforms):
    depth, width = lm_head.shape
    rows = draft_logits.shape[0]
    spans = rows // LANES
    flat = (spans, LANES)
    hbm = pl.BlockSpec(memory_space=pltpu.HBM)
    vmem = pl.BlockSpec(memory_space=pltpu.VMEM)
    stats = pl.pallas_call(
        main_kernel,
        out_shape=jax.ShapeDtypeStruct((5, *flat), jnp.float32),
        in_specs=[hbm] * 6,
        out_specs=vmem,
        scratch_shapes=[
            pltpu.VMEM(hidden.shape, jnp.bfloat16),
            pltpu.VMEM((depth // LANES, LANES), jnp.bfloat16),
            pltpu.VMEM((depth, width), jnp.bfloat16),
            pltpu.VMEM((rows, width), jnp.bfloat16),
            pltpu.VMEM(flat, jnp.int32),
            pltpu.VMEM(flat, jnp.int32),
            pltpu.VMEM((depth // LANES, SIDE, SIDE, SIDE, hidden.shape[0], LANES), jnp.bfloat16),
            pltpu.VMEM((SIDE, SIDE, SIDE, hidden.shape[0], width), jnp.float32),
            pltpu.VMEM((rows, width), jnp.float32),
            pltpu.VMEM((rows, width), jnp.float32),
            pltpu.VMEM((9, *flat), jnp.float32),
            pltpu.VMEM((3, SIDE, 3, *flat), jnp.float32),
            pltpu.VMEM((3, SIDE, 1, *flat), jnp.float32),
            pltpu.VMEM((2, SIDE**3, *flat), jnp.float32),
            pltpu.SemaphoreType.DMA((5,)),
            pltpu.SemaphoreType.DMA((len(PAIRS),)),
            pltpu.SemaphoreType.DMA((len(MESSAGES),)),
            pltpu.SemaphoreType.DMA((len(MESSAGES),)),
            pltpu.SemaphoreType.DMA((6, 3)),
            pltpu.SemaphoreType.DMA((6, 3)),
            pltpu.SemaphoreType.DMA((2, SIDE**3 - 1)),
            pltpu.SemaphoreType.DMA((2, SIDE**3 - 1)),
        ],
        compiler_params=pltpu.CompilerParams(
            collective_id=0, has_side_effects=True, vmem_limit_bytes=60 * 2**20
        ),
        name="gather_verify",
    )(
        hidden,
        norm_gain.reshape(depth // LANES, LANES),
        lm_head,
        draft_logits,
        draft_tokens.reshape(flat),
        tree_parents.reshape(flat),
    )
    outs = pl.pallas_call(
        tree_kernel,
        out_shape=[jax.ShapeDtypeStruct(flat, jnp.float32)] * 5,
        in_specs=[vmem] * 4,
        out_specs=[vmem] * 5,
        name="tree",
    )(stats, tree_parents.reshape(flat), node_depths.reshape(flat), uniforms.reshape(flat))
    return tuple(out.reshape(rows) for out in outs)


def solution(mesh):
    return jax.shard_map(
        body,
        mesh=mesh,
        in_specs=(
            P(("batch", "vocab"), None),
            P(),
            P(None, "vocab"),
            P("batch", "vocab"),
            P("batch"),
            P("batch"),
            P("batch"),
            P("batch"),
        ),
        out_specs=(P("batch"), P("batch"), P("batch"), P("batch"), P("batch")),
        check_vma=False,
    )
```

```python
import heapq
import itertools

import jax
import jax.numpy as jnp
from jax import lax
from jax.experimental import pallas as pl
from jax.experimental.pallas import tpu as pltpu
from jax.sharding import PartitionSpec as P

NODES = 64
DEPTH_MAX = 8
EPSILON = 1e-06
LANES = 128
SIDE = 4
MESH = pl.DeviceIdType.MESH

ROUTES = ((0, 1, 2), (1, 2, 0), (2, 0, 1))
GROUPS = (
    ((3, 6, 10), (3, 6, 10), (3, 6, 5, 3, 2)),
    ((3, 6, 10), (3, 6, 10), (3, 6, 5, 3, 2)),
    ((3, 6, 9), (3, 6, 9), (3, 6, 4, 3, 2)),
)


def offset(p, phase, g):
    return sum(sum(part[0]) for part in GROUPS[:p]) + sum(GROUPS[p][phase][:g])


def finer(p, phase, g):
    low = offset(p, phase, g)
    high = low + GROUPS[p][phase][g]
    return [k for k in range(len(GROUPS[p][phase + 1])) if low <= offset(p, phase + 1, k) < high]


def relay_sides():
    sides = {}
    for p, part in enumerate(GROUPS):
        for phase, sizes in enumerate(part):
            lean = 0
            for g in sorted(range(len(sizes)), key=lambda g: -sizes[g]):
                sides[p, g, phase] = 0 if lean <= 0 else 1
                lean += sizes[g] if lean <= 0 else -sizes[g]
    return sides


SIDES = relay_sides()


def kinds_sent(g, phase):
    return (2, 0, 1) if phase == 0 or g == 0 and phase < 2 else (0, 1)


def passed_on(message):
    p, g, phase, kind = message
    return kind == SIDES[p, g, phase] and 2 not in kinds_sent(g, phase)


DRAFT = (
    [(("stats", b), 0.45, 2.0 if b == 0 else 0.0) for b in range(8)]
    + [(("join", axis), 0.3, 12.0 if axis else 0.0) for axis in range(4)]
    + [(("probs", b), 0.2, 0.0) for b in range(8)]
)


def plan():
    rate, gap, latency = 44500.0, 0.15, 2.2
    free = {(a, d): 0.0 for a in range(3) for d in range(2)}
    coming, count, have, order, ready = [], itertools.count(), set(), [], []
    draft = list(DRAFT)

    def send(now, p, g, phase, kind):
        way = (ROUTES[p][phase], kind if kind < 2 else SIDES[p, g, phase])
        free[way] = max(now, free[way]) + gap + GROUPS[p][phase][g] * 4096 * SIDE**phase / rate
        heapq.heappush(coming, (free[way] + latency, next(count), (p, g, phase, kind)))

    now, last = 0.0, 0.0
    for g in range(len(GROUPS[0][0])):
        for p in range(3):
            for kind in kinds_sent(g, 0):
                send(now, p, g, 0, kind)
    while coming or ready or draft:
        due = last + draft[0][2] if draft else float("inf")
        if coming and coming[0][0] <= now or not ready and coming and coming[0][0] <= due:
            at, _, message = heapq.heappop(coming)
            now = max(now, at) + 0.05
            p, g, phase, kind = message
            have.add(message)
            order.append(("take", message))
            if passed_on(message):
                send(now, p, g, phase, 2)
            if all((p, g, phase, k) in have for k in range(3)):
                for k in finer(p, phase, g) if phase < 2 else ():
                    for way in kinds_sent(k, phase + 1):
                        send(now, p, k, phase + 1, way)
                    if phase == 1:
                        ready.append((p, k, 3))
            if phase == 2:
                ready.append((p, g, kind))
        elif draft and (due <= now or not ready):
            what, cost, _ = draft.pop(0)
            order.append(("draft", what))
            now = last = max(now, due) + cost
        else:
            p, g, kind = ready.pop(0)
            order.append(("multiply", (p, g, kind)))
            now += 0.2 + 0.08 * max(2, GROUPS[p][2][g])
    return order


ORDER = plan()
PAIRS = [key[:2] for kind, key in ORDER if kind == "multiply" and key[2] == 3]
MESSAGES = [m for kind, m in ORDER if kind == "take"]


def as_column(row):
    return jnp.transpose(jnp.broadcast_to(row, (LANES, LANES)))


def main_kernel(
    hidden_hbm, gain_hbm, head_hbm, draft_hbm, tokens_hbm, parents_hbm,
    out_ref,
    hidden_ref, gain_ref, head_ref, draft_ref, tokens_ref, parents_ref,
    rows_ref, logits_ref, weight_ref, draft_prob_ref, stat_ref, pair_ref, pick_ref, bank_ref,
    small_sem, head_sem, send_sem, take_sem, swap_send_sem, swap_take_sem, far_send_sem, far_take_sem,
):
    me = lax.axis_index("vocab")
    batch = lax.axis_index("batch")
    at = (me // 16, (me // 4) % 4, me % 4)
    stride = (16, 4, 1)
    width = weight_ref.shape[1]
    spans = weight_ref.shape[0] // LANES

    def peer(axis, step):
        return (me + (lax.rem(at[axis] + step, SIDE) - at[axis]) * stride[axis], batch)

    small = [
        pltpu.make_async_copy(src, dst, small_sem.at[k])
        for k, (src, dst) in enumerate(
            (
                (hidden_hbm, hidden_ref),
                (gain_hbm, gain_ref),
                (draft_hbm, draft_ref),
                (tokens_hbm, tokens_ref),
                (parents_hbm, parents_ref),
            )
        )
    ]
    for copy in small:
        copy.start()
    barrier = pltpu.get_barrier_semaphore()
    for axis in range(3):
        for step in (2, 1, 3):
            pl.semaphore_signal(barrier, inc=1, device_id=peer(axis, step), device_id_type=MESH)
    head_copies = {}
    for k, pair in enumerate(PAIRS):
        span = pl.ds(offset(pair[0], 2, pair[1]) * LANES, GROUPS[pair[0]][2][pair[1]] * LANES)
        head_copies[pair] = pltpu.make_async_copy(head_hbm.at[span], head_ref.at[span], head_sem.at[k])
        head_copies[pair].start()

    small[0].wait()
    small[1].wait()
    tiles = hidden_ref.shape[1] // LANES
    squares = jnp.zeros((16, LANES), jnp.float32)
    for k in range(tiles):
        part = hidden_ref[:, k * LANES : (k + 1) * LANES].astype(jnp.float32)
        squares += part * part
    scale = lax.rsqrt(jnp.sum(squares, axis=1, keepdims=True) / hidden_ref.shape[1] + EPSILON)
    for k in range(tiles):
        part = hidden_ref[:, k * LANES : (k + 1) * LANES].astype(jnp.float32)
        gain = gain_ref[k : k + 1, :].astype(jnp.float32)
        rows_ref[k, at[0], at[1], at[2]] = (part * scale * gain).astype(jnp.bfloat16)
    for y in range(SIDE):
        logits_ref[y] = jnp.zeros(logits_ref.shape[1:], jnp.float32)
    pl.semaphore_wait(barrier, 9)

    number = {m: k for k, m in enumerate(MESSAGES)}
    sent = []

    def message(p, g, phase, kind, taking):
        axis = ROUTES[p][phase]
        side = kind if kind < 2 else SIDES[p, g, phase]
        up = 1 if side == 0 else 3
        routed = kind == 2 and 2 in kinds_sent(g, phase)
        begun = (SIDE - up) * (2 if kind == 2 else 1) if taking else ((SIDE - up) if kind == 2 and not routed else 0)
        index = [pl.ds(offset(p, phase, g), GROUPS[p][phase][g]), *at]
        for done in range(phase):
            index[1 + ROUTES[p][done]] = pl.ds(0, SIDE)
        index[1 + axis] = lax.rem(at[axis] + begun, SIDE)
        block = rows_ref.at[tuple(index)]
        k = number[p, g, phase, kind]
        return pltpu.make_async_remote_copy(
            src_ref=block,
            dst_ref=block,
            send_sem=send_sem.at[k],
            recv_sem=take_sem.at[k],
            device_id=peer(axis, 2 if routed else up),
            device_id_type=MESH,
        )

    def send(*key):
        copy = message(*key, False)
        copy.start()
        sent.append(copy)

    def multiply(p, g, kind):
        first, many = offset(p, 2, g), GROUPS[p][2][g]
        if kind == 3:
            head_copies[p, g].wait()
        axis = ROUTES[p][2]
        plane = [slice(None)] * 3
        plane[axis] = lax.rem(at[axis] + (3, 1, 2, 0)[kind], SIDE)
        count = SIDE * SIDE * hidden_ref.shape[0]
        left = jnp.concatenate(
            [rows_ref[(first + k, *plane)].reshape(count, LANES) for k in range(many)], axis=1
        )
        product = jnp.dot(
            left, head_ref[first * LANES : (first + many) * LANES, :], preferred_element_type=jnp.float32
        )
        index = tuple(plane)
        logits_ref[index] += product.reshape(SIDE, SIDE, hidden_ref.shape[0], width)

    def put(ref, stage, axis, values):
        for k, value in enumerate(values):
            ref[stage, at[axis], k] = value

    def swap(ref, stage, number_of, axis):
        copies = []
        for step in (1, 2, 3):
            block = ref.at[stage, at[axis]]
            copy = pltpu.make_async_remote_copy(
                src_ref=block,
                dst_ref=block,
                send_sem=swap_send_sem.at[number_of, step - 1],
                recv_sem=swap_take_sem.at[number_of, step - 1],
                device_id=peer(axis, step),
                device_id_type=MESH,
            )
            copy.start()
            copies.append(copy)
        sent.extend(copies)
        return copies

    def taken(ref, stage, number_of, axis):
        for step in (1, 2, 3):
            block = ref.at[stage, lax.rem(at[axis] + SIDE - step, SIDE)]
            pltpu.make_async_remote_copy(
                src_ref=block,
                dst_ref=block,
                send_sem=swap_send_sem.at[number_of, step - 1],
                recv_sem=swap_take_sem.at[number_of, step - 1],
                device_id=peer(axis, step),
                device_id_type=MESH,
            ).wait_recv()

    def joined_pair(stage):
        tops = [pair_ref[stage, c, 0] for c in range(SIDE)]
        top = jnp.maximum(jnp.maximum(tops[0], tops[1]), jnp.maximum(tops[2], tops[3]))
        total = sum(pair_ref[stage, c, 1] * jnp.exp(tops[c] - top) for c in range(SIDE))
        return top, total, sum(pair_ref[stage, c, 2] for c in range(SIDE))

    shifts = sorted(
        (o for o in itertools.product(range(SIDE), repeat=3) if any(o)), key=lambda o: -sum(min(v, SIDE - v) for v in o)
    )

    places = [[lax.rem(at[axis] + step, SIDE) * stride[axis] for step in range(SIDE)] for axis in range(3)]

    def across(turn, k, back):
        steps = [(SIDE - step) % SIDE if back else step for step in shifts[k]]
        there = sum(places[axis][step] for axis, step in enumerate(steps))
        block = bank_ref.at[turn, there if back else me]
        return pltpu.make_async_remote_copy(
            src_ref=block,
            dst_ref=block,
            send_sem=far_send_sem.at[turn, k],
            recv_sem=far_take_sem.at[turn, k],
            device_id=(there, batch),
            device_id_type=MESH,
        )

    def cast(turn, value):
        bank_ref[turn, me] = value
        for k in range(len(shifts)):
            copy = across(turn, k, False)
            copy.start()
            sent.append(copy)

    def collected(turn):
        for k in range(len(shifts)):
            across(turn, k, True).wait_recv()
        return [bank_ref[turn, v] for v in range(len(shifts) + 1)]

    def joined_lse(values):
        top = values[0]
        for value in values[1:]:
            top = jnp.maximum(top, value)
        return top + jnp.log(sum(jnp.exp(value - top) for value in values))

    def rows_of(b):
        return pl.ds(pl.multiple_of(b * LANES, LANES), LANES)

    def logits_at(b, tile):
        block = logits_ref[b // 2, pl.ds(lax.rem(b, 2) * 2, 2), :, :, tile]
        return block.reshape(LANES, tile.stop - tile.start)

    def stat_row(k, b):
        return stat_ref[k, pl.ds(b, 1), :]

    def set_stat(k, b, value):
        stat_ref[k, pl.ds(b, 1), :] = value

    def down(matrix, combine):
        return combine(jnp.transpose(matrix), axis=0, keepdims=True)

    lane = lax.broadcasted_iota(jnp.int32, (LANES, LANES), 1).astype(jnp.float32)

    def pickers(b):
        parent = as_column(parents_ref[pl.ds(b, 1), :].astype(jnp.float32))
        below = (lax.broadcasted_iota(jnp.int32, (LANES, LANES), 0) // NODES * NODES).astype(jnp.float32)
        hot = jnp.where(parent + below == lane, 1.0, 0.0).astype(jnp.bfloat16)
        token = as_column((tokens_ref[pl.ds(b, 1), :] - me * width).astype(jnp.float32))
        return hot, token

    def picked(pieces, hot, token):
        total = jnp.zeros((LANES, LANES), jnp.float32)
        for c in range(width // 256):
            found = sum(
                jnp.dot(hot, piece, preferred_element_type=jnp.float32)
                for piece in pieces(slice(c * 256, (c + 1) * 256))
            )
            for half in range(2):
                here = found[:, half * LANES : (half + 1) * LANES]
                total += jnp.where(token == lane + float(c * 256 + half * LANES), here, 0.0)
        return total

    def column_tiles():
        return [slice(c * LANES, (c + 1) * LANES) for c in range(width // LANES)]

    def draft_stats(b, carry):
        rows = rows_of(b)
        top = jnp.full((LANES, LANES), -jnp.inf, jnp.float32)
        for tile in column_tiles():
            top = jnp.maximum(top, draft_ref[rows, tile].astype(jnp.float32))
        top = down(top, jnp.max)
        column = as_column(top)
        total = jnp.zeros((LANES, LANES), jnp.float32)
        for tile in column_tiles():
            total += jnp.exp(draft_ref[rows, tile].astype(jnp.float32) - column)
        set_stat(0, b, top)
        set_stat(1, b, down(total, jnp.sum))
        hot, token = pickers(b)
        set_stat(2, b, down(picked(lambda tile: [draft_ref[rows, tile]], hot, token), jnp.sum))
        return carry

    def draft_probs(b, carry):
        rows = rows_of(b)
        column = as_column(stat_row(6, b))
        for tile in column_tiles():
            draft_prob_ref[rows, tile] = jnp.exp(draft_ref[rows, tile].astype(jnp.float32) - column)
        return carry

    def target_stats(b, carry):
        rows = rows_of(b)
        top = jnp.full((LANES, LANES), -jnp.inf, jnp.float32)
        for tile in column_tiles():
            top = jnp.maximum(top, logits_at(b, tile))
        top = down(top, jnp.max)
        column = as_column(top)
        total = jnp.zeros((LANES, LANES), jnp.float32)
        for tile in column_tiles():
            weight = jnp.exp(logits_at(b, tile) - column)
            weight_ref[rows, tile] = weight
            total += weight
        set_stat(3, b, top)
        set_stat(4, b, down(total, jnp.sum))
        return carry

    def target_picks(b, carry):
        rows = rows_of(b)

        def pieces(tile):
            values = logits_at(b, tile)
            high = values.astype(jnp.bfloat16)
            rest = values - high.astype(jnp.float32)
            middle = rest.astype(jnp.bfloat16)
            low = (rest - middle.astype(jnp.float32)).astype(jnp.bfloat16)
            return high, middle, low

        hot, token = pickers(b)
        set_stat(5, b, down(picked(pieces, hot, token), jnp.sum))
        return carry

    def residuals(b, carry):
        rows = rows_of(b)
        factor = as_column(stat_row(7, b))
        total = jnp.zeros((LANES, LANES), jnp.float32)
        for tile in column_tiles():
            total += jnp.maximum(weight_ref[rows, tile] * factor - draft_prob_ref[rows, tile], 0.0)
        set_stat(8, b, down(total, jnp.sum))
        return carry

    def over(body, unroll):
        lax.fori_loop(0, spans, body, 0, unroll=unroll)

    def work_on_draft(what, which):
        if what == "stats":
            if which == 0:
                for copy in small[2:]:
                    copy.wait()
            draft_stats(which, 0)
        elif what == "probs":
            draft_probs(which, 0)
        else:
            if which:
                taken(pair_ref, which - 1, which - 1, which - 1)
            values = joined_pair(which - 1) if which else (stat_ref[0], stat_ref[1], stat_ref[2])
            if which < 3:
                put(pair_ref, which, which, values)
                swap(pair_ref, which, which, which)
            else:
                stat_ref[6] = values[0] + jnp.log(values[1])
                out_ref[1] = stat_ref[6]
                out_ref[4] = values[2]

    for g in range(len(GROUPS[0][0])):
        for p in range(3):
            for kind in kinds_sent(g, 0):
                send(p, g, 0, kind)
    have = set()
    for kind, key in ORDER:
        if kind == "multiply":
            multiply(*key)
        elif kind == "draft":
            work_on_draft(*key)
        else:
            message(*key, True).wait_recv()
            p, g, phase, way = key
            have.add(key)
            if passed_on(key):
                send(p, g, phase, 2)
            if phase < 2 and all((p, g, phase, k) in have for k in range(3)):
                for k in finer(p, phase, g):
                    for to in kinds_sent(k, phase + 1):
                        send(p, k, phase + 1, to)

    over(target_stats, spans)
    cast(0, stat_ref[3] + jnp.log(stat_ref[4]))
    over(target_picks, 2)
    def pick_sum(stage):
        taken(pick_ref, stage, 3 + stage, stage)
        return sum(pick_ref[stage, c, 0] for c in range(SIDE))

    put(pick_ref, 0, 0, (stat_ref[5],))
    swap(pick_ref, 0, 3, 0)
    early = len(sent) - len(shifts) - 3
    for copy in sent[:early]:
        copy.wait_send()
    del sent[:early]
    target_lse = joined_lse(collected(0))
    stat_ref[7] = jnp.exp(stat_ref[3] - target_lse)
    over(residuals, spans)
    cast(1, stat_ref[8])
    out_ref[0] = target_lse
    put(pick_ref, 1, 1, (pick_sum(0),))
    swap(pick_ref, 1, 4, 1)
    early = len(sent) - len(shifts) - 3
    for copy in sent[:early]:
        copy.wait_send()
    del sent[:early]
    put(pick_ref, 2, 2, (pick_sum(1),))
    swap(pick_ref, 2, 5, 2)
    out_ref[3] = pick_sum(2)
    out_ref[2] = sum(collected(1))
    for copy in sent:
        copy.wait_send()


def tree_kernel(stats_ref, parents_ref, depths_ref, uniforms_ref, lse_ref, token_ref, residual_ref, accept_ref, path_ref):
    lanes = lax.broadcasted_iota(jnp.int32, parents_ref.shape, 1)
    parent = lanes // NODES * NODES + parents_ref[...]

    def at_parent(vector):
        return jnp.take_along_axis(vector, parent, axis=1)

    target_lse = stats_ref[0]
    token_logprob = stats_ref[3] - at_parent(target_lse)
    draft_logprob = stats_ref[4] - at_parent(stats_ref[1])
    accept = jnp.exp(jnp.minimum(token_logprob - draft_logprob, 0.0)) - uniforms_ref[...]
    depths = depths_ref[...]
    path = jnp.ones(accept.shape, jnp.float32)
    for level in range(1, DEPTH_MAX + 1):
        path = jnp.where(depths == level, jnp.minimum(accept, at_parent(path)), path)
    lse_ref[...] = target_lse
    token_ref[...] = token_logprob
    residual_ref[...] = stats_ref[2]
    accept_ref[...] = accept
    path_ref[...] = path


def body(hidden, norm_gain, lm_head, draft_logits, draft_tokens, tree_parents, node_depths, uniforms):
    depth, width = lm_head.shape
    rows = draft_logits.shape[0]
    spans = rows // LANES
    flat = (spans, LANES)
    hbm = pl.BlockSpec(memory_space=pltpu.HBM)
    vmem = pl.BlockSpec(memory_space=pltpu.VMEM)
    stats = pl.pallas_call(
        main_kernel,
        out_shape=jax.ShapeDtypeStruct((5, *flat), jnp.float32),
        in_specs=[hbm] * 6,
        out_specs=vmem,
        scratch_shapes=[
            pltpu.VMEM(hidden.shape, jnp.bfloat16),
            pltpu.VMEM((depth // LANES, LANES), jnp.bfloat16),
            pltpu.VMEM((depth, width), jnp.bfloat16),
            pltpu.VMEM((rows, width), jnp.bfloat16),
            pltpu.VMEM(flat, jnp.int32),
            pltpu.VMEM(flat, jnp.int32),
            pltpu.VMEM((depth // LANES, SIDE, SIDE, SIDE, hidden.shape[0], LANES), jnp.bfloat16),
            pltpu.VMEM((SIDE, SIDE, SIDE, hidden.shape[0], width), jnp.float32),
            pltpu.VMEM((rows, width), jnp.float32),
            pltpu.VMEM((rows, width), jnp.float32),
            pltpu.VMEM((9, *flat), jnp.float32),
            pltpu.VMEM((3, SIDE, 3, *flat), jnp.float32),
            pltpu.VMEM((3, SIDE, 1, *flat), jnp.float32),
            pltpu.VMEM((2, SIDE**3, *flat), jnp.float32),
            pltpu.SemaphoreType.DMA((5,)),
            pltpu.SemaphoreType.DMA((len(PAIRS),)),
            pltpu.SemaphoreType.DMA((len(MESSAGES),)),
            pltpu.SemaphoreType.DMA((len(MESSAGES),)),
            pltpu.SemaphoreType.DMA((6, 3)),
            pltpu.SemaphoreType.DMA((6, 3)),
            pltpu.SemaphoreType.DMA((2, SIDE**3 - 1)),
            pltpu.SemaphoreType.DMA((2, SIDE**3 - 1)),
        ],
        compiler_params=pltpu.CompilerParams(
            collective_id=0, has_side_effects=True, vmem_limit_bytes=60 * 2**20
        ),
        name="gather_verify",
    )(
        hidden,
        norm_gain.reshape(depth // LANES, LANES),
        lm_head,
        draft_logits,
        draft_tokens.reshape(flat),
        tree_parents.reshape(flat),
    )
    outs = pl.pallas_call(
        tree_kernel,
        out_shape=[jax.ShapeDtypeStruct(flat, jnp.float32)] * 5,
        in_specs=[vmem] * 4,
        out_specs=[vmem] * 5,
        name="tree",
    )(stats, tree_parents.reshape(flat), node_depths.reshape(flat), uniforms.reshape(flat))
    return tuple(out.reshape(rows) for out in outs)


def solution(mesh):
    return jax.shard_map(
        body,
        mesh=mesh,
        in_specs=(
            P(("batch", "vocab"), None),
            P(),
            P(None, "vocab"),
            P("batch", "vocab"),
            P("batch"),
            P("batch"),
            P("batch"),
            P("batch"),
        ),
        out_specs=(P("batch"), P("batch"), P("batch"), P("batch"), P("batch")),
        check_vma=False,
    )
```
